32 devices in a mesh: dp: 1 (over z), tp: 4 (over y), cp: 8 (over x, core).
Axes of the slice: x: 4, y: 4, z: 1, core: 2. Of those that a mesh axis runs over, the one named last changes fastest.
The devices are a block of a 4x4x8 slice.
Arguments:
- x: bfloat16 [4096, 3072], P(('dp', 'cp'))
- doc_id: int32 [4096], P(('dp', 'cp'))
- pos_in_doc: int32 [4096], P(('dp', 'cp'))
- norm_gain: float32 [3072], replicated
- w_q: bfloat16 [3072, 3072], P(None, 'tp')
- w_k: bfloat16 [3072, 1024], P(None, 'tp')
- w_v: bfloat16 [3072, 1024], P(None, 'tp')
- w_o: bfloat16 [3072, 3072], P('tp')
- inv_freq: float32 [64], replicated
Outputs:
- output 1: bfloat16 [4096, 3072], P(('dp', 'cp'))
- output 2: bfloat16 [4096, 8, 128], P(('dp', 'cp'), 'tp')
- output 3: bfloat16 [4096, 8, 128], P(('dp', 'cp'), 'tp')
All inputs are finite; a program needn't handle non-finite values.
Results may differ from the reference program's by a relative error of at most 0.00161997.
Values are sent between devices in bfloat16 or wider.
A program may use at most 768 MiB of HBM per device.

```python
import jax
import jax.numpy as jnp
from jax import lax

TOKENS = 4096
CP_SIZE = 8
D_MODEL = 3072
Q_HEADS = 24
KV_HEADS = 8
HEAD_DIM = 128
DOC_LEN = 96
ROPE_THETA = 500000
QUERY_ROWS = 128

PIECE_LEN = TOKENS // (2 * CP_SIZE)
GROUP_SIZE = Q_HEADS // KV_HEADS
MAX_DOCS = TOKENS // (DOC_LEN // 2) + 2


def to_stored(glob_arr):
    pieces = glob_arr.reshape((2 * CP_SIZE, PIECE_LEN) + glob_arr.shape[1:])
    paired = jnp.stack([pieces[:CP_SIZE], pieces[CP_SIZE:][::-1]], axis=1)
    return paired.reshape(glob_arr.shape)


def draw_documents(doc_key):
    key_long, key_before, key_after = jax.random.split(doc_key, 3)
    first_piece = (DOC_LEN - 2) // PIECE_LEN + 1
    long_piece = jax.random.randint(key_long, (), first_piece, 2 * CP_SIZE)
    long_start = long_piece * PIECE_LEN - DOC_LEN + 1
    long_end = long_start + DOC_LEN
    lens_before = jax.random.randint(key_before, (MAX_DOCS,), DOC_LEN // 2, DOC_LEN + 1)
    lens_after = jax.random.randint(key_after, (MAX_DOCS,), DOC_LEN // 2, DOC_LEN + 1)
    starts_before = jnp.cumsum(lens_before)
    starts_after = long_end + jnp.cumsum(lens_after) - lens_after
    start_marks = jnp.zeros((TOKENS,), jnp.int32).at[0].set(1).at[long_start].set(1)
    start_marks = start_marks.at[jnp.where(starts_before < long_start, starts_before, TOKENS)].set(1, mode='drop')
    start_marks = start_marks.at[starts_after].set(1, mode='drop')
    doc_glob = jnp.cumsum(start_marks) - 1
    tok_index = jnp.arange(TOKENS)
    pos_glob = tok_index - lax.cummax(tok_index * start_marks, axis=0)
    return doc_glob.astype(jnp.int32), pos_glob.astype(jnp.int32)


def normal_weight(weight_key, fan_in, fan_out):
    return (jax.random.normal(weight_key, (fan_in, fan_out), jnp.float32) * fan_in ** -0.5).astype(jnp.bfloat16)


def setup_inputs(seed: int = 0, part: int = 0) -> dict:
    part_key = jax.random.fold_in(jax.random.key(seed), part)
    key_doc, key_noise, key_drift = jax.random.split(part_key, 3)
    shared = jax.random.split(jax.random.key(seed + 1), 6)
    doc_glob, pos_glob = draw_documents(key_doc)
    pos_ratio = pos_glob.astype(jnp.float32) / DOC_LEN
    drift_dir = jax.random.normal(key_drift, (D_MODEL,), jnp.float32)
    x_noise = jax.random.normal(key_noise, (TOKENS, D_MODEL), jnp.float32)
    x_glob = x_noise + 3.0 * pos_ratio[:, None] * drift_dir[None, :]
    norm_gain = 1.0 + 0.25 * jax.random.normal(shared[0], (D_MODEL,), jnp.float32)
    w_q = normal_weight(shared[1], D_MODEL, Q_HEADS * HEAD_DIM)
    w_k = normal_weight(shared[2], D_MODEL, KV_HEADS * HEAD_DIM)
    w_v = normal_weight(shared[3], D_MODEL, KV_HEADS * HEAD_DIM)
    w_o = normal_weight(shared[4], Q_HEADS * HEAD_DIM, D_MODEL)
    base_freq = ROPE_THETA ** (-jnp.arange(0, HEAD_DIM, 2, dtype=jnp.float32) / HEAD_DIM)
    inv_freq = base_freq * jnp.exp(0.1 * jax.random.normal(shared[5], (HEAD_DIM // 2,), jnp.float32))
    return {'x': to_stored(x_glob).astype(jnp.bfloat16), 'doc_id': to_stored(doc_glob), 'pos_in_doc': to_stored(pos_glob), 'norm_gain': norm_gain, 'w_q': w_q, 'w_k': w_k, 'w_v': w_v, 'w_o': w_o, 'inv_freq': inv_freq}


def apply_rope(vectors, cos_t, sin_t):
    half_dim = vectors.shape[-1] // 2
    lower_half = vectors[..., :half_dim].astype(jnp.float32)
    upper_half = vectors[..., half_dim:].astype(jnp.float32)
    turned = jnp.concatenate([lower_half * cos_t - upper_half * sin_t, upper_half * cos_t + lower_half * sin_t], axis=-1)
    return turned.astype(jnp.bfloat16)


def reference(x, doc_id, pos_in_doc, norm_gain, w_q, w_k, w_v, w_o, inv_freq):
    x_f32 = x.astype(jnp.float32)
    inv_rms = lax.rsqrt(jnp.mean(x_f32 * x_f32, axis=-1, keepdims=True) + 1e-5)
    normed = (x_f32 * inv_rms * norm_gain).astype(jnp.bfloat16)
    q_new = jnp.dot(normed, w_q, preferred_element_type=jnp.float32).astype(jnp.bfloat16).reshape(TOKENS, KV_HEADS, GROUP_SIZE, HEAD_DIM)
    k_new = jnp.dot(normed, w_k, preferred_element_type=jnp.float32).astype(jnp.bfloat16).reshape(TOKENS, KV_HEADS, HEAD_DIM)
    v_new = jnp.dot(normed, w_v, preferred_element_type=jnp.float32).astype(jnp.bfloat16).reshape(TOKENS, KV_HEADS, HEAD_DIM)
    rope_angle = pos_in_doc.astype(jnp.float32)[:, None] * inv_freq[None, :]
    cos_t = jnp.cos(rope_angle)
    sin_t = jnp.sin(rope_angle)
    q_rot = apply_rope(q_new, cos_t[:, None, None, :], sin_t[:, None, None, :])
    k_rot = apply_rope(k_new, cos_t[:, None, :], sin_t[:, None, :])
    tok_index = to_stored(jnp.arange(TOKENS))
    k_f32 = k_rot.astype(jnp.float32)
    v_f32 = v_new.astype(jnp.float32)
    blocks = TOKENS // QUERY_ROWS

    def attend(block_args):
        q_blk, doc_blk, idx_blk = block_args
        scores = jnp.einsum('qngd,knd->ngqk', q_blk.astype(jnp.float32), k_f32) * (HEAD_DIM ** -0.5)
        visible = (doc_blk[:, None] == doc_id[None, :]) & (tok_index[None, :] <= idx_blk[:, None])
        scores = jnp.where(visible, scores, -1e30)
        attn_probs = jax.nn.softmax(scores, axis=-1).astype(jnp.bfloat16).astype(jnp.float32)
        return jnp.einsum('ngqk,knd->qngd', attn_probs, v_f32).astype(jnp.bfloat16)

    attn_out = lax.map(attend, (q_rot.reshape(blocks, QUERY_ROWS, KV_HEADS, GROUP_SIZE, HEAD_DIM), doc_id.reshape(blocks, QUERY_ROWS), tok_index.reshape(blocks, QUERY_ROWS)))
    mixed_out = jnp.dot(attn_out.reshape(TOKENS, Q_HEADS * HEAD_DIM), w_o, preferred_element_type=jnp.float32)
    y_out = (x_f32 + mixed_out).astype(jnp.bfloat16)
    return (y_out, k_rot, v_new)
```

```python
import functools

import jax
import jax.numpy as jnp
from jax import lax
from jax.experimental import pallas as pl
from jax.experimental.pallas import tpu as pltpu
from jax.sharding import PartitionSpec as P

MESH = pl.DeviceIdType.MESH
F32 = jnp.float32
BF16 = jnp.bfloat16
HALO = 128
BLK = 128
TILE = 256
NEG = -1e30


class Copies:
    def __init__(self, send_sems, recv_sems):
        self.send_sems, self.recv_sems, self.made = send_sems, recv_sems, {}

    def start(self, name, src, dst, device):
        slot = len(self.made)
        copy = pltpu.make_async_remote_copy(src_ref=src, dst_ref=dst, send_sem=self.send_sems.at[slot], recv_sem=self.recv_sems.at[slot], device_id=device, device_id_type=MESH)
        self.made[name] = copy
        copy.start()

    def arrived(self, name):
        self.made[name].wait_recv()

    def drain(self):
        for copy in self.made.values():
            copy.wait_send()


def layer_kernel(cp_size, tp_size, x_hbm, pos_hbm, gain_hbm, wq_hbm, wk_hbm, wv_hbm, wo_hbm, freq_hbm,
                 y_hbm, k_hbm, v_hbm, far_ref,
                 x_v, h_v, wq_v, wk_v, wv_v, w_all, transit, o_all, y_v, q_v, k_win, v_win, k_out, v_out,
                 pos_v, gain_v, freq_v, cos_v, sin_v, posb_v, pos_all, load_sems, send_sems, recv_sems):
    rows, d_model = x_v.shape
    piece = rows // 2
    half = d_model // 2
    q_cols = q_v.shape[1]
    head_dim = freq_v.shape[1] * 2
    kv_heads = k_win.shape[2] // head_dim
    group = q_cols // (kv_heads * head_dim)
    gcols = group * head_dim
    share = q_cols // cp_size
    part = share // 2

    me_c = lax.axis_index("cp")
    me_t = lax.axis_index("tp")
    up_t = {"tp": lax.rem(me_t + 1, tp_size)}
    dn_t = {"tp": lax.rem(me_t + tp_size - 1, tp_size)}
    up_x = {"cp": lax.rem(me_c + 2, cp_size)}
    dn_x = {"cp": lax.rem(me_c + cp_size - 2, cp_size)}
    mate = {"cp": me_c + 1 - 2 * lax.rem(me_c, 2)}
    nxt = {"cp": lax.rem(me_c + 1, cp_size)}
    prv = {"cp": lax.rem(me_c + cp_size - 1, cp_size)}
    mine = lax.rem(me_t, 2)
    other = 1 - mine
    my_cols = pl.multiple_of(mine * half, half)
    other_cols = pl.multiple_of(other * half, half)

    loads = {}

    def load(name, src, dst):
        copy = pltpu.make_async_copy(src, dst, load_sems.at[len(loads)])
        loads[name] = copy
        copy.start()

    load("pos", pos_hbm, pos_v)
    load("freq", freq_hbm, freq_v)
    load("gain", gain_hbm, gain_v)
    for c in range(rows // BLK):
        load(("x", c), x_hbm.at[pl.ds(c * BLK, BLK)], x_v.at[pl.ds(c * BLK, BLK)])
    load("wk", wk_hbm, wk_v)
    load("wv", wv_hbm, wv_v)
    load("wq", wq_hbm, wq_v)
    load("wo", wo_hbm.at[:, pl.ds(my_cols, half)], w_all.at[0])

    barrier = pltpu.get_barrier_semaphore()
    for d in range(1, cp_size):
        pl.semaphore_signal(barrier, inc=1, device_id={"cp": lax.rem(me_c + d, cp_size)}, device_id_type=MESH)
    for peer in (up_t, dn_t):
        pl.semaphore_signal(barrier, inc=1, device_id=peer, device_id_type=MESH)
    pl.semaphore_wait(barrier, cp_size + 1)

    rc = Copies(send_sems, recv_sems)
    row0 = pl.multiple_of(me_c * share, share)
    row1 = pl.multiple_of(me_c * share + part, part)

    def share_of(who):
        return pl.ds(pl.multiple_of(who * share, share), share)

    def part_of(who, i):
        return pl.ds(pl.multiple_of(who * share + i * part, part), part)

    rc.start("w_up", wo_hbm.at[pl.ds(row0, share), pl.ds(other_cols, half)], w_all.at[3, pl.ds(row0, share)], up_t)
    rc.start("w_dn", wo_hbm.at[pl.ds(row0, share), pl.ds(other_cols, half)], w_all.at[1, pl.ds(row0, share)], dn_t)
    rc.start("t_up", wo_hbm.at[pl.ds(row0, part), pl.ds(my_cols, half)], transit.at[0], up_t)
    rc.start("t_dn", wo_hbm.at[pl.ds(row1, part), pl.ds(my_cols, half)], transit.at[1], dn_t)
    for d in range(1, cp_size):
        rc.start(("pos", d), pos_hbm, pos_all.at[cp_size - d], {"cp": lax.rem(me_c + d, cp_size)})

    loads["pos"].wait()
    loads["freq"].wait()
    pos_all[0] = pos_v[...]
    freq = jnp.concatenate([freq_v[...], freq_v[...]], axis=1)
    sign = jnp.where(lax.broadcasted_iota(jnp.int32, (1, head_dim), 1) < head_dim // 2, -1.0, 1.0).astype(F32)
    for c in range(rows // BLK):
        pos_rows = jnp.transpose(jnp.broadcast_to(pos_v[pl.ds(c, 1), :], (BLK, BLK)))
        posb_v[pl.ds(c * BLK, BLK), :] = pos_rows
        angle = pos_rows.astype(F32) * freq
        cos_v[pl.ds(c * BLK, BLK), :] = jnp.cos(angle)
        sin_v[pl.ds(c * BLK, BLK), :] = jnp.sin(angle) * sign

    loads["gain"].wait()
    for c in range(rows // BLK):
        loads[("x", c)].wait()

        def norm(i, carry):
            at = pl.ds(pl.multiple_of(c * BLK + i * 32, 32), 32)
            x_f32 = x_v[at, :].astype(F32)
            inv_rms = lax.rsqrt(jnp.mean(x_f32 * x_f32, axis=-1, keepdims=True) + 1e-5)
            h_v[at, :] = (x_f32 * inv_rms * gain_v[...]).astype(BF16)
            return carry

        lax.fori_loop(0, BLK // 32, norm, 0)

    def rope(raw, c):
        at = pl.ds(c * BLK, BLK)
        vec = raw.astype(F32)
        return (vec * cos_v[at, :] + pltpu.roll(vec, head_dim // 2, 1) * sin_v[at, :]).astype(BF16)

    def window_at(c):
        return c * BLK // piece, pl.ds(HALO + c * BLK % piece, BLK)

    loads["wk"].wait()
    k_new = jnp.dot(h_v[...], wk_v[...], preferred_element_type=F32).astype(BF16)
    for c in range(rows // BLK):
        p, at = window_at(c)
        heads = []
        for n in range(kv_heads):
            rot = rope(k_new[c * BLK:(c + 1) * BLK, n * head_dim:(n + 1) * head_dim], c)
            k_win[p, at, n * head_dim:(n + 1) * head_dim] = rot
            heads.append(rot)
        k_out[pl.ds(c * BLK, BLK)] = jnp.stack(heads, axis=1)
    tail = pl.ds(piece, HALO)
    halo = pl.ds(0, HALO)
    rc.start("hk_a", k_win.at[0, tail], k_win.at[0, halo], nxt)
    rc.start("hk_b", k_win.at[1, tail], k_win.at[1, halo], prv)
    loads["wv"].wait()
    v_new = jnp.dot(h_v[...], wv_v[...], preferred_element_type=F32).astype(BF16)
    for c in range(rows // BLK):
        p, at = window_at(c)
        v_win[p, at, :] = v_new[c * BLK:(c + 1) * BLK]
        v_out[pl.ds(c * BLK, BLK)] = jnp.stack([v_new[c * BLK:(c + 1) * BLK, n * head_dim:(n + 1) * head_dim] for n in range(kv_heads)], axis=1)
    rc.start("hv_a", v_win.at[0, tail], v_win.at[0, halo], nxt)
    rc.start("hv_b", v_win.at[1, tail], v_win.at[1, halo], prv)
    load("k_out", k_out, k_hbm)
    load("v_out", v_out, v_hbm)

    def spread_own(r):
        at = share_of(me_c)
        rc.start(("xu", r), w_all.at[r, at], w_all.at[r, at], up_x)
        rc.start(("xd", r), w_all.at[r, at], w_all.at[r, at], dn_x)
        rc.start(("m0", r), w_all.at[r, at], w_all.at[r, at], mate)

    def spread_near(r):
        lo, hi = share_of(dn_x["cp"]), share_of(up_x["cp"])
        rc.arrived(("xu", r))
        rc.start(("fu", r), w_all.at[r, part_of(dn_x["cp"], 0)], w_all.at[r, part_of(dn_x["cp"], 0)], up_x)
        rc.start(("m1", r), w_all.at[r, lo], w_all.at[r, lo], mate)
        rc.arrived(("xd", r))
        rc.start(("fd", r), w_all.at[r, part_of(up_x["cp"], 1)], w_all.at[r, part_of(up_x["cp"], 1)], dn_x)
        rc.start(("m2", r), w_all.at[r, hi], w_all.at[r, hi], mate)

    def spread_far(r):
        far = lax.rem(me_c + cp_size // 2, cp_size)
        rc.arrived(("fu", r))
        rc.arrived(("fd", r))
        rc.start(("m3", r), w_all.at[r, share_of(far)], w_all.at[r, share_of(far)], mate)

    rc.arrived("t_up")
    rc.start("t_up2", transit.at[0], w_all.at[2, pl.ds(row0, part)], up_t)
    rc.arrived("t_dn")
    rc.start("t_dn2", transit.at[1], w_all.at[2, pl.ds(row1, part)], dn_t)
    rc.arrived("w_up")
    rc.arrived("w_dn")
    spread_own(3)
    spread_own(1)

    loads["wq"].wait()

    def project_q(i, carry):
        at = pl.ds(pl.multiple_of(i * TILE, TILE), TILE)
        q_new = jnp.dot(h_v[...], wq_v[:, at], preferred_element_type=F32).astype(BF16)
        for c in range(rows // BLK):
            for n in range(TILE // head_dim):
                rot = rope(q_new[c * BLK:(c + 1) * BLK, n * head_dim:(n + 1) * head_dim], c)
                q_v[pl.ds(c * BLK, BLK), pl.ds(pl.multiple_of(i * TILE + n * head_dim, head_dim), head_dim)] = rot
        return carry

    lax.fori_loop(0, q_cols // TILE, project_q, 0)

    rc.arrived("t_up2")
    rc.arrived("t_dn2")
    spread_own(2)

    for name in ("hk_a", "hk_b", "hv_a", "hv_b"):
        rc.arrived(name)

    @pl.when(me_c == cp_size - 1)
    def _():
        k_win[1, 0:HALO, :] = k_win[0, piece:piece + HALO, :]
        v_win[1, 0:HALO, :] = v_win[0, piece:piece + HALO, :]

    score_scale = head_dim ** -0.5
    for p in range(2):
        for n in range(kv_heads):
            cols = slice(n * head_dim, (n + 1) * head_dim)
            for b in range(piece // BLK):
                keys = HALO + (b + 1) * BLK
                at = pl.ds(p * piece + b * BLK, BLK)
                q_blk = jnp.concatenate([q_v[at, (n * group + g) * head_dim:(n * group + g + 1) * head_dim] for g in range(group)], axis=0)
                scores = lax.dot_general(q_blk, k_win[p, 0:keys, cols], (((1,), (1,)), ((), ())), preferred_element_type=F32) * score_scale
                key = lax.broadcasted_iota(jnp.int32, (BLK, keys), 1) - HALO
                row = lax.broadcasted_iota(jnp.int32, (BLK, keys), 0) + b * BLK
                back = jnp.concatenate([posb_v[at, :]] * (keys // BLK), axis=1)
                visible = (key <= row) & (key >= row - back)
                scores = jnp.where(visible[None], scores.reshape(group, BLK, keys), NEG)
                top = jnp.max(scores, axis=-1, keepdims=True)
                weights = jnp.exp(scores - top)
                probs = (weights / jnp.sum(weights, axis=-1, keepdims=True)).astype(BF16).reshape(group * BLK, keys)
                o_blk = jnp.dot(probs, v_win[p, 0:keys, cols], preferred_element_type=F32).astype(BF16)
                for g in range(group):
                    o_all[0, at, (n * group + g) * head_dim:(n * group + g + 1) * head_dim] = o_blk[g * BLK:(g + 1) * BLK]
            block = (pl.ds(p * piece, piece), pl.ds(n * gcols, gcols))
            rc.start(("ou", p, n), o_all.at[(0,) + block], o_all.at[(3,) + block], up_t)
            rc.start(("od", p, n), o_all.at[(0,) + block], o_all.at[(1,) + block], dn_t)

    def forward_o(p):
        first = (pl.ds(p * piece, piece), pl.ds(0, gcols))
        last = (pl.ds(p * piece, piece), pl.ds((kv_heads - 1) * gcols, gcols))
        rc.arrived(("ou", p, 0))
        rc.start(("fou", p), o_all.at[(3,) + first], o_all.at[(2,) + first], up_t)
        rc.arrived(("od", p, 0))
        rc.arrived(("od", p, 1))
        rc.start(("fod", p), o_all.at[(1,) + last], o_all.at[(2,) + last], dn_t)
        rc.arrived(("ou", p, 1))

    for d in range(1, cp_size):
        rc.arrived(("pos", d))
    sub = lax.broadcasted_iota(jnp.int32, pos_all.shape, 1)
    lane = lax.broadcasted_iota(jnp.int32, pos_all.shape, 2)
    first_tok = (lane == 0) & ((sub == 0) | (sub == piece // BLK))
    far_ref[0] = jnp.max(jnp.where(first_tok, pos_all[...], 0))

    forward_o(0)
    spread_near(3)
    spread_near(1)
    forward_o(1)
    spread_near(2)
    for r in (3, 1, 2):
        spread_far(r)
    loads["wo"].wait()
    for r in (3, 1, 2):
        for i in range(4):
            rc.arrived(("m%d" % i, r))

    for p in range(2):
        rc.arrived(("fou", p))
        rc.arrived(("fod", p))
        at = pl.ds(p * piece, piece)

        def out_tile(i, carry):
            cols = pl.ds(pl.multiple_of(i * TILE, TILE), TILE)
            acc = jnp.dot(o_all[0, at, :], w_all[0, :, cols], preferred_element_type=F32)
            for r in range(1, 4):
                acc += jnp.dot(o_all[r, at, :], w_all[r, :, cols], preferred_element_type=F32)
            x_cols = pl.ds(pl.multiple_of(my_cols + i * TILE, TILE), TILE)
            y_v[at, cols] = (x_v[at, x_cols].astype(F32) + acc).astype(BF16)
            return carry

        lax.fori_loop(0, half // TILE, out_tile, 0)
        lo, hi = pl.ds(p * piece, BLK), pl.ds(p * piece + BLK, BLK)
        cols = pl.ds(my_cols, half)
        rc.start(("yd", p), y_v.at[lo], y_hbm.at[lo, cols], dn_t)
        rc.start(("yu", p), y_v.at[hi], y_hbm.at[hi, cols], up_t)
        load(("y", p), y_v.at[at], y_hbm.at[at, cols])

    for name in ("k_out", "v_out", ("y", 0), ("y", 1)):
        loads[name].wait()
    rc.drain()
    for p in range(2):
        rc.arrived(("yd", p))
        rc.arrived(("yu", p))


def fused_layer(cp_size, tp_size, x_in, pos_in_doc, norm_gain, w_q, w_k, w_v, w_o, inv_freq):
    rows, d_model = x_in.shape
    q_cols, kv_cols = w_q.shape[1], w_k.shape[1]
    head_dim = 2 * inv_freq.shape[0]
    kv_heads = kv_cols // head_dim
    piece, half = rows // 2, d_model // 2
    vm = pltpu.VMEM
    copies = 6 + (cp_size - 1) + 4 + 3 * 9 + 8 + 4 + 4 + 4
    any_spec = pl.BlockSpec(memory_space=pl.ANY)
    return pl.pallas_call(
        functools.partial(layer_kernel, cp_size, tp_size),
        name="fused_layer",
        out_shape=[
            jax.ShapeDtypeStruct((rows, d_model), BF16),
            jax.ShapeDtypeStruct((rows, kv_heads, head_dim), BF16),
            jax.ShapeDtypeStruct((rows, kv_heads, head_dim), BF16),
            jax.ShapeDtypeStruct((1,), jnp.int32),
        ],
        in_specs=[any_spec] * 8,
        out_specs=[any_spec] * 3 + [pl.BlockSpec(memory_space=pltpu.SMEM)],
        scratch_shapes=[
            vm((rows, d_model), BF16), vm((rows, d_model), BF16),
            vm(w_q.shape, BF16), vm(w_k.shape, BF16), vm(w_v.shape, BF16),
            vm((tp_size, q_cols, half), BF16), vm((2, q_cols // cp_size // 2, half), BF16),
            vm((tp_size, rows, q_cols), BF16), vm((rows, half), BF16), vm((rows, q_cols), BF16),
            vm((2, HALO + piece, kv_cols), BF16), vm((2, HALO + piece, kv_cols), BF16),
            vm((rows, kv_heads, head_dim), BF16), vm((rows, kv_heads, head_dim), BF16),
            vm((rows // BLK, BLK), jnp.int32), vm((1, d_model), F32), vm((1, head_dim // 2), F32),
            vm((rows, head_dim), F32), vm((rows, head_dim), F32), vm((rows, BLK), jnp.int32),
            vm((cp_size, rows // BLK, BLK), jnp.int32),
            pltpu.SemaphoreType.DMA((20,)),
            pltpu.SemaphoreType.DMA((copies,)), pltpu.SemaphoreType.DMA((copies,)),
        ],
        compiler_params=pltpu.CompilerParams(collective_id=0, has_side_effects=True, vmem_limit_bytes=60 * 1024 * 1024),
    )(x_in, pos_in_doc.reshape(rows // BLK, BLK), norm_gain.reshape(1, d_model), w_q, w_k, w_v, w_o, inv_freq.reshape(1, head_dim // 2))


def gather_kernel(axis, size, part_hbm, all_hbm, load_sem, send_sems, recv_sems):
    me = lax.axis_index(axis)
    barrier = pltpu.get_barrier_semaphore()
    for d in range(1, size):
        pl.semaphore_signal(barrier, inc=1, device_id={axis: lax.rem(me + d, size)}, device_id_type=MESH)
    pl.semaphore_wait(barrier, size - 1)
    own = pltpu.make_async_copy(part_hbm, all_hbm.at[me], load_sem)
    own.start()
    copies = []
    for d in range(1, size):
        copies.append(pltpu.make_async_remote_copy(src_ref=part_hbm, dst_ref=all_hbm.at[me], send_sem=send_sems.at[d - 1], recv_sem=recv_sems.at[d - 1], device_id={axis: lax.rem(me + d, size)}, device_id_type=MESH))
        copies[-1].start()
    for copy in copies:
        copy.wait()
    own.wait()


def gather(part, axis, size, collective_id):
    any_spec = pl.BlockSpec(memory_space=pl.ANY)
    return pl.pallas_call(
        functools.partial(gather_kernel, axis, size),
        name="gather_%d" % collective_id,
        out_shape=jax.ShapeDtypeStruct((size,) + part.shape, part.dtype),
        in_specs=[any_spec],
        out_specs=any_spec,
        scratch_shapes=[pltpu.SemaphoreType.DMA, pltpu.SemaphoreType.DMA((size - 1,)), pltpu.SemaphoreType.DMA((size - 1,))],
        compiler_params=pltpu.CompilerParams(collective_id=collective_id, has_side_effects=True),
    )(part)


def rope_ref(vectors, cos_t, sin_t):
    half_dim = vectors.shape[-1] // 2
    lower_half = vectors[..., :half_dim].astype(F32)
    upper_half = vectors[..., half_dim:].astype(F32)
    return jnp.concatenate([lower_half * cos_t - upper_half * sin_t, upper_half * cos_t + lower_half * sin_t], axis=-1).astype(BF16)


def global_index(stored_pos, local_rows, cp_size):
    piece_len = local_rows // 2
    owner = stored_pos // local_rows
    within = stored_pos % local_rows
    piece_id = jnp.where(within < piece_len, owner, 2 * cp_size - 1 - owner)
    return piece_id * piece_len + within % piece_len


def general_y(cp_size, tp_size, x_in, pos_in_doc, norm_gain, w_q, w_o, inv_freq, k_rot, v_new):
    rows, kv_heads, head_dim = k_rot.shape
    tokens = rows * cp_size
    x_f32 = x_in.astype(F32)
    inv_rms = lax.rsqrt(jnp.mean(x_f32 * x_f32, axis=-1, keepdims=True) + 1e-5)
    normed = (x_f32 * inv_rms * norm_gain).astype(BF16)
    q_new = jnp.dot(normed, w_q, preferred_element_type=F32).astype(BF16).reshape(rows, kv_heads, -1, head_dim)
    angle = pos_in_doc.astype(F32)[:, None] * inv_freq[None, :]
    q_rot = rope_ref(q_new, jnp.cos(angle)[:, None, None, :], jnp.sin(angle)[:, None, None, :])
    keys = gather(k_rot.reshape(rows, kv_heads * head_dim), "cp", cp_size, 1).reshape(tokens, kv_heads, head_dim)
    vals = gather(v_new.reshape(rows, kv_heads * head_dim), "cp", cp_size, 2).reshape(tokens, kv_heads, head_dim)
    q_idx = global_index(lax.axis_index("cp") * rows + jnp.arange(rows), rows, cp_size)
    key_idx = global_index(jnp.arange(tokens), rows, cp_size)

    def attend(block_args):
        q_blk, idx_blk, pos_blk = block_args
        scores = jnp.einsum("qngd,knd->ngqk", q_blk, keys, preferred_element_type=F32) * head_dim ** -0.5
        visible = (key_idx[None, :] >= (idx_blk - pos_blk)[:, None]) & (key_idx[None, :] <= idx_blk[:, None])
        probs = jax.nn.softmax(jnp.where(visible, scores, NEG), axis=-1).astype(BF16)
        return jnp.einsum("ngqk,knd->qngd", probs, vals, preferred_element_type=F32).astype(BF16)

    blocks = rows // BLK
    o_own = lax.map(attend, (q_rot.reshape(blocks, BLK, kv_heads, -1, head_dim), q_idx.reshape(blocks, BLK), pos_in_doc.reshape(blocks, BLK))).reshape(rows, -1)
    o_parts = gather(o_own, "tp", tp_size, 3)
    w_parts = gather(w_o, "tp", tp_size, 4)
    mixed = jnp.einsum("trc,tcd->rd", o_parts, w_parts, preferred_element_type=F32)
    return (x_f32 + mixed).astype(BF16)


def solution(mesh):
    cp_size, tp_size = mesh.shape["cp"], mesh.shape["tp"]

    def local_step(x_in, doc_id, pos_in_doc, norm_gain, w_q, w_k, w_v, w_o, inv_freq):
        y_out, k_rot, v_new, far = fused_layer(cp_size, tp_size, x_in, pos_in_doc, norm_gain, w_q, w_k, w_v, w_o, inv_freq)

        def redo(state):
            y_new = general_y(cp_size, tp_size, x_in, pos_in_doc, norm_gain, w_q, w_o, inv_freq, k_rot, v_new)
            return jnp.zeros_like(state[0]), y_new

        _, y_out = lax.while_loop(lambda state: state[0] > HALO, redo, (far[0], y_out))
        return y_out, k_rot, v_new

    row_spec = P(("dp", "cp"))
    in_specs = (P(("dp", "cp"), None), row_spec, row_spec, P(), P(None, "tp"), P(None, "tp"), P(None, "tp"), P("tp", None), P())
    out_specs = (P(("dp", "cp"), None), P(("dp", "cp"), "tp", None), P(("dp", "cp"), "tp", None))
    return jax.shard_map(local_step, mesh=mesh, in_specs=in_specs, out_specs=out_specs, check_vma=False)
```

```python
import functools
import math

import jax
import jax.numpy as jnp
from jax import lax
from jax.experimental import pallas as pl
from jax.experimental.pallas import tpu as pltpu
from jax.sharding import PartitionSpec as P

MESH = pl.DeviceIdType.MESH
F32 = jnp.float32
BF16 = jnp.bfloat16
HALO = 128
BLK = 128
GROUPS = 3
NEG = -1e30


class Copies:
    def __init__(self, send_sems, recv_sems, ruler):
        self.send_sems, self.recv_sems, self.ruler = send_sems, recv_sems, ruler
        self.made, self.send_slots, self.recv_slots, self.sent, self.due = {}, {}, {}, {}, {}

    def start(self, name, src, dst, device, send_batch=None, recv_batch=None):
        send_slot = self.send_slots.setdefault(send_batch or name, len(self.send_slots))
        recv_slot = self.recv_slots.setdefault(recv_batch or name, len(self.recv_slots))
        copy = pltpu.make_async_remote_copy(src_ref=src, dst_ref=dst, send_sem=self.send_sems.at[send_slot], recv_sem=self.recv_sems.at[recv_slot], device_id=device, device_id_type=MESH)
        size = math.prod(src.shape)
        if send_batch is None:
            self.made[name] = (copy, True)
        else:
            self.made[name] = (copy, False)
            self.sent[send_batch] = self.sent.get(send_batch, 0) + size
        if recv_batch is not None:
            self.due[recv_batch] = self.due.get(recv_batch, 0) + size
        copy.start()

    def wait_size(self, sem, size):
        slabs, depth, width = self.ruler.shape
        total = size // width
        count = next(n for n in range(1, slabs + 1) if total % (16 * n) == 0 and total // n <= depth)
        ref = self.ruler.at[pl.ds(0, count), pl.ds(0, total // count)]
        pltpu.make_async_copy(ref, ref, sem).wait()

    def arrived(self, name):
        self.made[name][0].wait_recv()

    def batch_arrived(self, batch):
        self.wait_size(self.recv_sems.at[self.recv_slots[batch]], self.due[batch])

    def drain(self):
        for copy, alone in self.made.values():
            if alone:
                copy.wait_send()
        for batch, size in self.sent.items():
            self.wait_size(self.send_sems.at[self.send_slots[batch]], size)


def layer_kernel(cp_size, tp_size, x_hbm, pos_hbm, gain_hbm, wq_hbm, wk_hbm, wv_hbm, wo_hbm, freq_hbm,
                 y_out, k_out, v_out, far_hbm,
                 x_v, h_v, wq_v, wkv_v, w_all, w_share, o_all, q_v, k_win, v_win,
                 pos_v, gain_v, freq_v, cos_v, sin_v, posb_v, pos_all, far_s, load_sems, send_sems, recv_sems):
    rows, d_model = x_v.shape
    piece = rows // 2
    half = d_model // 2
    q_cols = q_v.shape[1]
    head_dim = freq_v.shape[1] * 2
    kv_cols = k_win.shape[2]
    kv_heads = kv_cols // head_dim
    group = q_cols // (kv_heads * head_dim)
    gcols = group * head_dim
    share = q_cols // cp_size
    part = share // 2

    me_c = lax.axis_index("cp")
    me_t = lax.axis_index("tp")
    up_t = {"tp": lax.rem(me_t + 1, tp_size)}
    dn_t = {"tp": lax.rem(me_t + tp_size - 1, tp_size)}
    op_t = {"tp": lax.rem(me_t + tp_size // 2, tp_size)}
    up_x = {"cp": lax.rem(me_c + 2, cp_size)}
    dn_x = {"cp": lax.rem(me_c + cp_size - 2, cp_size)}
    mate = {"cp": me_c + 1 - 2 * lax.rem(me_c, 2)}
    nxt = {"cp": lax.rem(me_c + 1, cp_size)}
    prv = {"cp": lax.rem(me_c + cp_size - 1, cp_size)}
    mine = lax.rem(me_t, 2)
    other = 1 - mine
    my_cols = pl.multiple_of(mine * half, half)
    other_cols = pl.multiple_of(other * half, half)

    row0 = pl.multiple_of(me_c * share, share)
    loads = {}

    def load(name, src, dst):
        copy = pltpu.make_async_copy(src, dst, load_sems.at[len(loads)])
        loads[name] = copy
        copy.start()

    load("pos", pos_hbm, pos_v)
    load("freq", freq_hbm, freq_v)
    load("gain", gain_hbm, gain_v)
    load("share", wo_hbm.at[pl.ds(row0, share)], w_share)
    for c in range(rows // BLK):
        load(("x", c), x_hbm.at[pl.ds(c * BLK, BLK)], x_v.at[pl.ds(c * BLK, BLK)])
    load("wk", wk_hbm, wkv_v.at[:, pl.ds(0, kv_cols)])
    load("wv", wv_hbm, wkv_v.at[:, pl.ds(kv_cols, kv_cols)])
    load("wq", wq_hbm, wq_v)
    load("wo", wo_hbm.at[:, pl.ds(my_cols, half)], w_all.at[0])

    barrier = pltpu.get_barrier_semaphore()
    for d in range(1, cp_size):
        pl.semaphore_signal(barrier, inc=1, device_id={"cp": lax.rem(me_c + d, cp_size)}, device_id_type=MESH)
    for peer in (up_t, dn_t, op_t):
        pl.semaphore_signal(barrier, inc=1, device_id=peer, device_id_type=MESH)

    rc = Copies(send_sems, recv_sems, w_all)
    def share_of(who):
        return pl.ds(pl.multiple_of(who * share, share), share)

    def part_of(who, i):
        return pl.ds(pl.multiple_of(who * share + i * part, part), part)

    gw = half // GROUPS

    def group_of(start, g):
        return pl.ds(pl.multiple_of(start + g * gw, gw), gw)

    def send_shares(g):
        here = pl.ds(g * gw, gw)
        rc.start(("w_up", g), w_share.at[:, group_of(other_cols, g)], w_all.at[3, pl.ds(row0, share), here], up_t, "w")
        rc.start(("w_dn", g), w_share.at[:, group_of(other_cols, g)], w_all.at[1, pl.ds(row0, share), here], dn_t, "w")
        rc.start(("w_op", g), w_share.at[:, group_of(my_cols, g)], w_all.at[2, pl.ds(row0, share), here], op_t, "w")

    def spread_own(r, g):
        rc.arrived((("w_dn", "w_op", "w_up")[r - 1], g))
        at = (r, share_of(me_c), pl.ds(g * gw, gw))
        rc.start(("xu", r, g), w_all.at[at], w_all.at[at], up_x, "w")
        rc.start(("xd", r, g), w_all.at[at], w_all.at[at], dn_x, "w")
        rc.start(("m0", r, g), w_all.at[at], w_all.at[at], mate, "w", ("m", g))

    def spread_near(r, g):
        here = pl.ds(g * gw, gw)
        for name, fwd, to_mate, source, i, onward in (("xu", "fu", "m1", dn_x, 0, up_x), ("xd", "fd", "m2", up_x, 1, dn_x)):
            at = (r, part_of(source["cp"], i), here)
            rc.arrived((name, r, g))
            rc.start((fwd, r, g), w_all.at[at], w_all.at[at], onward, "w")
            at = (r, share_of(source["cp"]), here)
            rc.start((to_mate, r, g), w_all.at[at], w_all.at[at], mate, "w", ("m", g))

    def spread_far(r, g):
        at = (r, share_of(lax.rem(me_c + cp_size // 2, cp_size)), pl.ds(g * gw, gw))
        rc.arrived(("fu", r, g))
        rc.arrived(("fd", r, g))
        rc.start(("m3", r, g), w_all.at[at], w_all.at[at], mate, "w", ("m", g))

    loads["pos"].wait()
    loads["freq"].wait()
    pos_all[0] = pos_v[...]
    freq = jnp.concatenate([freq_v[...], freq_v[...]], axis=1)
    sign = jnp.where(lax.broadcasted_iota(jnp.int32, (1, head_dim), 1) < head_dim // 2, -1.0, 1.0).astype(F32)
    left = lax.broadcasted_iota(jnp.int32, (BLK, head_dim), 1) < head_dim // 2
    for c in range(rows // BLK):
        posb_v[pl.ds(c * BLK, BLK), :] = jnp.transpose(jnp.broadcast_to(pos_v[pl.ds(c, 1), :], (BLK, BLK)))
    for c in range(rows // BLK // 2):
        at, up = pl.ds(c * BLK, BLK), pl.ds(piece + c * BLK, BLK)
        angle = jnp.where(left, posb_v[at, :], posb_v[up, :]).astype(F32) * freq
        for out, both in ((cos_v, jnp.cos(angle)), (sin_v, jnp.sin(angle))):
            turned = pltpu.roll(both, head_dim // 2, 1)
            scale = sign if out is sin_v else 1.0
            out[at, :] = jnp.where(left, both, turned) * scale
            out[up, :] = jnp.where(left, turned, both) * scale

    loads["gain"].wait()
    for c in range(rows // BLK):
        loads[("x", c)].wait()

        def norm(i, carry):
            at = pl.ds(pl.multiple_of(c * BLK + i * 32, 32), 32)
            x_f32 = x_v[at, :].astype(F32)
            inv_rms = lax.rsqrt(jnp.mean(x_f32 * x_f32, axis=-1, keepdims=True) + 1e-5)
            h_v[at, :] = (x_f32 * inv_rms * gain_v[...]).astype(BF16)
            return carry

        lax.fori_loop(0, BLK // 32, norm, 0)
        if c == 1:
            pl.semaphore_wait(barrier, cp_size + 2)
            loads["share"].wait()
            send_shares(0)

    def rope(raw, c):
        at = pl.ds(c * BLK, BLK)
        vec = raw.astype(F32)
        return (vec * cos_v[at, :] + pltpu.roll(vec, head_dim // 2, 1) * sin_v[at, :]).astype(BF16)

    def window_at(c):
        return c * BLK // piece, pl.ds(HALO + c * BLK % piece, BLK)

    loads["wk"].wait()
    loads["wv"].wait()
    kv_new = jnp.dot(h_v[...], wkv_v[...], preferred_element_type=F32).astype(BF16)
    for c in range(rows // BLK):
        p, at = window_at(c)
        new = kv_new[c * BLK:(c + 1) * BLK]
        for n in range(kv_heads):
            k_win[p, at, n * head_dim:(n + 1) * head_dim] = rope(new[:, n * head_dim:(n + 1) * head_dim], c)
        v_win[p, at, :] = new[:, kv_cols:]
    tail = pl.ds(piece, HALO)
    halo = pl.ds(0, HALO)
    rc.start("hk_a", k_win.at[0, tail], k_win.at[0, halo], nxt)
    rc.start("hk_b", k_win.at[1, tail], k_win.at[1, halo], prv)
    rc.start("hv_a", v_win.at[0, tail], v_win.at[0, halo], nxt)
    rc.start("hv_b", v_win.at[1, tail], v_win.at[1, halo], prv)

    send_shares(1)
    for d in range(1, cp_size):
        rc.start(("pos", d), pos_hbm, pos_all.at[cp_size - d], {"cp": lax.rem(me_c + d, cp_size)})

    loads["wq"].wait()

    q_new = jnp.dot(h_v[...], wq_v[...], preferred_element_type=F32).astype(BF16)
    for c in range(rows // BLK):
        for n in range(q_cols // head_dim):
            cols = slice(n * head_dim, (n + 1) * head_dim)
            q_v[pl.ds(c * BLK, BLK), cols] = rope(q_new[c * BLK:(c + 1) * BLK, cols], c)

    send_shares(2)
    for r in (3, 1, 2):
        spread_own(r, 0)
    for name in ("hk_a", "hk_b", "hv_a", "hv_b"):
        rc.arrived(name)

    @pl.when(me_c == cp_size - 1)
    def _():
        k_win[1, 0:HALO, :] = k_win[0, piece:piece + HALO, :]
        v_win[1, 0:HALO, :] = v_win[0, piece:piece + HALO, :]

    def send_o(p, n):
        block = (pl.ds(p * piece, piece), pl.ds(n * gcols, gcols))
        rc.start(("ou", p, n), o_all.at[(0,) + block], o_all.at[(3,) + block], up_t, "oy")
        rc.start(("od", p, n), o_all.at[(0,) + block], o_all.at[(1,) + block], dn_t, "oy")

    score_scale = head_dim ** -0.5
    for p in range(2):
        for n in range(kv_heads):
            cols = slice(n * head_dim, (n + 1) * head_dim)
            for b in range(piece // BLK):
                keys = HALO + (b + 1) * BLK
                at = pl.ds(p * piece + b * BLK, BLK)
                q_blk = jnp.concatenate([q_v[at, (n * group + g) * head_dim:(n * group + g + 1) * head_dim] for g in range(group)], axis=0)
                scores = lax.dot_general(q_blk, k_win[p, 0:keys, cols], (((1,), (1,)), ((), ())), preferred_element_type=F32) * score_scale
                key = lax.broadcasted_iota(jnp.int32, (BLK, keys), 1) - HALO
                row = lax.broadcasted_iota(jnp.int32, (BLK, keys), 0) + b * BLK
                back = jnp.concatenate([posb_v[at, :]] * (keys // BLK), axis=1)
                visible = (key <= row) & (key >= row - back)
                scores = jnp.where(visible[None], scores.reshape(group, BLK, keys), NEG)
                top = jnp.max(scores, axis=-1, keepdims=True)
                weights = jnp.exp(scores - top)
                probs = (weights / jnp.sum(weights, axis=-1, keepdims=True)).astype(BF16).reshape(group * BLK, keys)
                o_blk = jnp.dot(probs, v_win[p, 0:keys, cols], preferred_element_type=F32).astype(BF16)
                for g in range(group):
                    o_all[0, at, (n * group + g) * head_dim:(n * group + g + 1) * head_dim] = o_blk[g * BLK:(g + 1) * BLK]
            send_o(p, n)

    def forward_o(p):
        first = (pl.ds(p * piece, piece), pl.ds(0, gcols))
        last = (pl.ds(p * piece, piece), pl.ds((kv_heads - 1) * gcols, gcols))
        rc.arrived(("ou", p, 0))
        rc.start(("fou", p), o_all.at[(3,) + first], o_all.at[(2,) + first], up_t, "oy")
        rc.arrived(("od", p, 0))
        rc.arrived(("od", p, 1))
        rc.start(("fod", p), o_all.at[(1,) + last], o_all.at[(2,) + last], dn_t, "oy")
        rc.arrived(("ou", p, 1))

    def out_tile(p, g):
        at = pl.ds(p * piece, piece)
        cols = pl.ds(g * gw, gw)
        acc = jnp.dot(o_all[0, at, :], w_all[0, :, cols], preferred_element_type=F32)
        for r in range(1, tp_size):
            acc += jnp.dot(o_all[r, at, :], w_all[r, :, cols], preferred_element_type=F32)
        x_cols = group_of(my_cols, g)
        y_out[at, x_cols] = (x_v[at, x_cols].astype(F32) + acc).astype(BF16)
        lo, hi = pl.ds(p * piece, BLK), pl.ds(p * piece + BLK, BLK)
        rc.start(("yd", p, g), y_out.at[lo, x_cols], y_out.at[lo, x_cols], dn_t, "oy")
        rc.start(("yu", p, g), y_out.at[hi, x_cols], y_out.at[hi, x_cols], up_t, "oy")

    for r in (3, 1, 2):
        spread_own(r, 1)
    for win, out in ((k_win, k_out), (v_win, v_out)):
        for c in range(rows // BLK):
            p, at = window_at(c)
            out[pl.ds(c * BLK, BLK)] = jnp.stack([win[p, at, n * head_dim:(n + 1) * head_dim] for n in range(kv_heads)], axis=1)
    for d in range(1, cp_size):
        rc.arrived(("pos", d))
    sub = lax.broadcasted_iota(jnp.int32, pos_all.shape, 1)
    lane = lax.broadcasted_iota(jnp.int32, pos_all.shape, 2)
    first_tok = (lane == 0) & ((sub == 0) | (sub == piece // BLK))
    far_s[0] = jnp.max(jnp.where(first_tok, pos_all[...], 0))
    load("far", far_s, far_hbm)

    for r in (3, 1, 2):
        spread_near(r, 0)
    for r in (3, 1, 2):
        spread_own(r, 2)
    for r in (3, 1, 2):
        spread_near(r, 1)
    forward_o(0)
    for r in (3, 1, 2):
        spread_far(r, 0)
    for r in (3, 1, 2):
        spread_near(r, 2)
    forward_o(1)
    for r in (3, 1, 2):
        spread_far(r, 1)
    loads["wo"].wait()
    rc.batch_arrived(("m", 0))
    rc.arrived(("fou", 0))
    rc.arrived(("fod", 0))
    out_tile(0, 0)
    rc.batch_arrived(("m", 1))
    out_tile(0, 1)
    for r in (3, 1, 2):
        spread_far(r, 2)
    rc.batch_arrived(("m", 2))
    out_tile(0, 2)
    rc.arrived(("fou", 1))
    rc.arrived(("fod", 1))
    for g in range(GROUPS):
        out_tile(1, g)

    loads["far"].wait()
    rc.drain()
    for p in range(2):
        for g in range(GROUPS):
            rc.arrived(("yd", p, g))
            rc.arrived(("yu", p, g))


def fused_layer(cp_size, tp_size, x_in, pos_in_doc, norm_gain, w_q, w_k, w_v, w_o, inv_freq):
    rows, d_model = x_in.shape
    q_cols, kv_cols = w_q.shape[1], w_k.shape[1]
    head_dim = 2 * inv_freq.shape[0]
    kv_heads = kv_cols // head_dim
    piece, half = rows // 2, d_model // 2
    vm = pltpu.VMEM
    copies = 3 * GROUPS + (cp_size - 1) + 4 + 3 * GROUPS * 4 + GROUPS + 8 + 4 + 4 * GROUPS
    any_spec = pl.BlockSpec(memory_space=pl.ANY)
    return pl.pallas_call(
        functools.partial(layer_kernel, cp_size, tp_size),
        name="fused_layer",
        out_shape=[
            vm((rows, d_model), BF16),
            vm((rows, kv_heads, head_dim), BF16),
            vm((rows, kv_heads, head_dim), BF16),
            jax.ShapeDtypeStruct((1,), jnp.int32),
        ],
        in_specs=[pl.BlockSpec(memory_space=pltpu.HBM)] * 8,
        out_specs=[pl.BlockSpec(memory_space=pltpu.VMEM)] * 3 + [any_spec],
        scratch_shapes=[
            vm((rows, d_model), BF16), vm((rows, d_model), BF16),
            vm(w_q.shape, BF16), vm((d_model, 2 * kv_cols), BF16),
            vm((tp_size, q_cols, half), BF16), vm((q_cols // cp_size, d_model), BF16),
            vm((tp_size, rows, q_cols), BF16), vm((rows, q_cols), BF16),
            vm((2, HALO + piece, kv_cols), BF16), vm((2, HALO + piece, kv_cols), BF16),
            vm((rows // BLK, BLK), jnp.int32), vm((1, d_model), F32), vm((1, head_dim // 2), F32),
            vm((rows, head_dim), F32), vm((rows, head_dim), F32), vm((rows, BLK), jnp.int32),
            vm((cp_size, rows // BLK, BLK), jnp.int32),
            pltpu.SMEM((1,), jnp.int32),
            pltpu.SemaphoreType.DMA((13,)),
            pltpu.SemaphoreType.DMA((2 + 4 + cp_size - 1,)), pltpu.SemaphoreType.DMA((copies,)),
        ],
        compiler_params=pltpu.CompilerParams(collective_id=0, has_side_effects=True, vmem_limit_bytes=59 * 1024 * 1024),
    )(x_in, pos_in_doc.reshape(rows // BLK, BLK), norm_gain.reshape(1, d_model), w_q, w_k, w_v, w_o, inv_freq.reshape(1, head_dim // 2))


def store_kernel(y_v, k_v, v_v, y_hbm, k_hbm, v_hbm, sems):
    copies = [pltpu.make_async_copy(k_v, k_hbm, sems.at[0]), pltpu.make_async_copy(v_v, v_hbm, sems.at[1])]
    for i in range(4):
        at = pl.ds(i * y_v.shape[0] // 4, y_v.shape[0] // 4)
        copies.append(pltpu.make_async_copy(y_v.at[at], y_hbm.at[at], sems.at[2 + i]))
    for copy in copies:
        copy.start()
    for copy in copies:
        copy.wait()


def store_outputs(y_v, k_v, v_v):
    return pl.pallas_call(
        store_kernel,
        name="store_outputs",
        out_shape=[jax.ShapeDtypeStruct(a.shape, a.dtype) for a in (y_v, k_v, v_v)],
        in_specs=[pl.BlockSpec(memory_space=pltpu.VMEM)] * 3,
        out_specs=[pl.BlockSpec(memory_space=pltpu.HBM)] * 3,
        scratch_shapes=[pltpu.SemaphoreType.DMA((6,))],
        compiler_params=pltpu.CompilerParams(vmem_limit_bytes=1024 * 1024),
    )(y_v, k_v, v_v)


def gather_kernel(axis, size, part_hbm, all_hbm, load_sem, send_sems, recv_sems):
    me = lax.axis_index(axis)
    barrier = pltpu.get_barrier_semaphore()
    for d in range(1, size):
        pl.semaphore_signal(barrier, inc=1, device_id={axis: lax.rem(me + d, size)}, device_id_type=MESH)
    pl.semaphore_wait(barrier, size - 1)
    own = pltpu.make_async_copy(part_hbm, all_hbm.at[me], load_sem)
    own.start()
    copies = []
    for d in range(1, size):
        copies.append(pltpu.make_async_remote_copy(src_ref=part_hbm, dst_ref=all_hbm.at[me], send_sem=send_sems.at[d - 1], recv_sem=recv_sems.at[d - 1], device_id={axis: lax.rem(me + d, size)}, device_id_type=MESH))
        copies[-1].start()
    for copy in copies:
        copy.wait()
    own.wait()


def gather(part, axis, size, collective_id):
    any_spec = pl.BlockSpec(memory_space=pl.ANY)
    return pl.pallas_call(
        functools.partial(gather_kernel, axis, size),
        name="gather_%d" % collective_id,
        out_shape=jax.ShapeDtypeStruct((size,) + part.shape, part.dtype),
        in_specs=[any_spec],
        out_specs=any_spec,
        scratch_shapes=[pltpu.SemaphoreType.DMA, pltpu.SemaphoreType.DMA((size - 1,)), pltpu.SemaphoreType.DMA((size - 1,))],
        compiler_params=pltpu.CompilerParams(collective_id=collective_id, has_side_effects=True),
    )(part)


def rope_ref(vectors, cos_t, sin_t):
    half_dim = vectors.shape[-1] // 2
    lower_half = vectors[..., :half_dim].astype(F32)
    upper_half = vectors[..., half_dim:].astype(F32)
    return jnp.concatenate([lower_half * cos_t - upper_half * sin_t, upper_half * cos_t + lower_half * sin_t], axis=-1).astype(BF16)


def global_index(stored_pos, local_rows, cp_size):
    piece_len = local_rows // 2
    owner = stored_pos // local_rows
    within = stored_pos % local_rows
    piece_id = jnp.where(within < piece_len, owner, 2 * cp_size - 1 - owner)
    return piece_id * piece_len + within % piece_len


def general_y(cp_size, tp_size, x_in, pos_in_doc, norm_gain, w_q, w_o, inv_freq, k_rot, v_new):
    rows, kv_heads, head_dim = k_rot.shape
    tokens = rows * cp_size
    x_f32 = x_in.astype(F32)
    inv_rms = lax.rsqrt(jnp.mean(x_f32 * x_f32, axis=-1, keepdims=True) + 1e-5)
    normed = (x_f32 * inv_rms * norm_gain).astype(BF16)
    q_new = jnp.dot(normed, w_q, preferred_element_type=F32).astype(BF16).reshape(rows, kv_heads, -1, head_dim)
    angle = pos_in_doc.astype(F32)[:, None] * inv_freq[None, :]
    q_rot = rope_ref(q_new, jnp.cos(angle)[:, None, None, :], jnp.sin(angle)[:, None, None, :])
    keys = gather(k_rot.reshape(rows, kv_heads * head_dim), "cp", cp_size, 1).reshape(tokens, kv_heads, head_dim)
    vals = gather(v_new.reshape(rows, kv_heads * head_dim), "cp", cp_size, 2).reshape(tokens, kv_heads, head_dim)
    q_idx = global_index(lax.axis_index("cp") * rows + jnp.arange(rows), rows, cp_size)
    key_idx = global_index(jnp.arange(tokens), rows, cp_size)

    def attend(block_args):
        q_blk, idx_blk, pos_blk = block_args
        scores = jnp.einsum("qngd,knd->ngqk", q_blk, keys, preferred_element_type=F32) * head_dim ** -0.5
        visible = (key_idx[None, :] >= (idx_blk - pos_blk)[:, None]) & (key_idx[None, :] <= idx_blk[:, None])
        probs = jax.nn.softmax(jnp.where(visible, scores, NEG), axis=-1).astype(BF16)
        return jnp.einsum("ngqk,knd->qngd", probs, vals, preferred_element_type=F32).astype(BF16)

    blocks = rows // BLK
    o_own = lax.map(attend, (q_rot.reshape(blocks, BLK, kv_heads, -1, head_dim), q_idx.reshape(blocks, BLK), pos_in_doc.reshape(blocks, BLK))).reshape(rows, -1)
    o_parts = gather(o_own, "tp", tp_size, 3)
    w_parts = gather(w_o, "tp", tp_size, 4)
    mixed = jnp.einsum("trc,tcd->rd", o_parts, w_parts, preferred_element_type=F32)
    return (x_f32 + mixed).astype(BF16)


def solution(mesh):
    cp_size, tp_size = mesh.shape["cp"], mesh.shape["tp"]

    def local_step(x_in, doc_id, pos_in_doc, norm_gain, w_q, w_k, w_v, w_o, inv_freq):
        y_out, k_rot, v_new, far = fused_layer(cp_size, tp_size, x_in, pos_in_doc, norm_gain, w_q, w_k, w_v, w_o, inv_freq)
        y_out, k_rot, v_new = store_outputs(y_out, k_rot, v_new)

        def redo(state):
            y_new = general_y(cp_size, tp_size, x_in, pos_in_doc, norm_gain, w_q, w_o, inv_freq, k_rot, v_new)
            return jnp.zeros_like(state[0]), y_new

        _, y_out = lax.while_loop(lambda state: state[0] > HALO, redo, (far[0], y_out))
        return y_out, k_rot, v_new

    row_spec = P(("dp", "cp"))
    in_specs = (P(("dp", "cp"), None), row_spec, row_spec, P(), P(None, "tp"), P(None, "tp"), P(None, "tp"), P("tp", None), P())
    out_specs = (P(("dp", "cp"), None), P(("dp", "cp"), "tp", None), P(("dp", "cp"), "tp", None))
    return jax.shard_map(local_step, mesh=mesh, in_specs=in_specs, out_specs=out_specs, check_vma=False)
```

```python
import functools
import math

import jax
import jax.numpy as jnp
from jax import lax
from jax.experimental import pallas as pl
from jax.experimental.pallas import tpu as pltpu
from jax.sharding import PartitionSpec as P

MESH = pl.DeviceIdType.MESH
F32 = jnp.float32
BF16 = jnp.bfloat16
HALO = 128
BLK = 128
GROUPS = 3
EXTRA = 3
BATCH = ("w", "w", "w", "e")
NEG = -1e30


class Copies:
    def __init__(self, send_sems, recv_sems, rulers):
        self.send_sems, self.recv_sems, self.rulers = send_sems, recv_sems, rulers
        self.made, self.send_slots, self.recv_slots, self.sent, self.due = {}, {}, {}, {}, {}

    def start(self, name, src, dst, device, send_batch=None, recv_batch=None):
        send_slot = self.send_slots.setdefault(send_batch or name, len(self.send_slots))
        recv_slot = self.recv_slots.setdefault(recv_batch or name, len(self.recv_slots))
        copy = pltpu.make_async_remote_copy(src_ref=src, dst_ref=dst, send_sem=self.send_sems.at[send_slot], recv_sem=self.recv_sems.at[recv_slot], device_id=device, device_id_type=MESH)
        size = math.prod(src.shape)
        if send_batch is None:
            self.made[name] = (copy, True)
        else:
            self.made[name] = (copy, False)
            self.sent[send_batch] = self.sent.get(send_batch, 0) + size
        if recv_batch is not None:
            self.due[recv_batch] = self.due.get(recv_batch, 0) + size
        copy.start()

    def wait_size(self, sem, size):
        fits = []
        for ruler in self.rulers:
            slabs, depth, width = ruler.shape
            fits += [(ruler, n, size // width // n) for n in range(1, slabs + 1) if size % (16 * n * width) == 0 and size // width // n <= depth]
        ruler, count, deep = fits[0]
        ref = ruler.at[pl.ds(0, count), pl.ds(0, deep)]
        pltpu.make_async_copy(ref, ref, sem).wait()

    def arrived(self, name):
        self.made[name][0].wait_recv()

    def batch_arrived(self, batch):
        self.wait_size(self.recv_sems.at[self.recv_slots[batch]], self.due[batch])

    def drain(self):
        for copy, alone in self.made.values():
            if alone:
                copy.wait_send()
        for batch, size in self.sent.items():
            self.wait_size(self.send_sems.at[self.send_slots[batch]], size)


def layer_kernel(cp_size, tp_size, x_hbm, pos_hbm, gain_hbm, wq_hbm, wk_hbm, wv_hbm, wo_hbm, freq_hbm,
                 y_out, k_out, v_out, far_hbm,
                 x_v, h_v, wq_v, wkv_v, w_all, w_ext, w_share, o_all, q_v, k_win, v_win,
                 pos_v, gain_v, freq_v, cos_v, sin_v, posb_v, pos_all, far_s, load_sems, send_sems, recv_sems):
    rows, d_model = x_v.shape
    piece = rows // 2
    half = d_model // 2
    q_cols = q_v.shape[1]
    head_dim = freq_v.shape[1] * 2
    kv_cols = k_win.shape[2]
    kv_heads = kv_cols // head_dim
    group = q_cols // (kv_heads * head_dim)
    gcols = group * head_dim
    share = q_cols // cp_size
    part = share // 2

    me_c = lax.axis_index("cp")
    me_t = lax.axis_index("tp")
    up_t = {"tp": lax.rem(me_t + 1, tp_size)}
    dn_t = {"tp": lax.rem(me_t + tp_size - 1, tp_size)}
    op_t = {"tp": lax.rem(me_t + tp_size // 2, tp_size)}
    up_x = {"cp": lax.rem(me_c + 2, cp_size)}
    dn_x = {"cp": lax.rem(me_c + cp_size - 2, cp_size)}
    mate = {"cp": me_c + 1 - 2 * lax.rem(me_c, 2)}
    nxt = {"cp": lax.rem(me_c + 1, cp_size)}
    prv = {"cp": lax.rem(me_c + cp_size - 1, cp_size)}
    mine = lax.rem(me_t, 2)
    other = 1 - mine
    my_cols = pl.multiple_of(mine * half, half)
    other_cols = pl.multiple_of(other * half, half)

    row0 = pl.multiple_of(me_c * share, share)
    loads = {}

    def load(name, src, dst):
        copy = pltpu.make_async_copy(src, dst, load_sems.at[len(loads)])
        loads[name] = copy
        copy.start()

    load("pos", pos_hbm, pos_v)
    load("freq", freq_hbm, freq_v)
    load("gain", gain_hbm, gain_v)
    load("share", wo_hbm.at[pl.ds(row0, share)], w_share)
    for c in range(rows // BLK):
        load(("x", c), x_hbm.at[pl.ds(c * BLK, BLK)], x_v.at[pl.ds(c * BLK, BLK)])
    load("wk", wk_hbm, wkv_v.at[:, pl.ds(0, kv_cols)])
    load("wv", wv_hbm, wkv_v.at[:, pl.ds(kv_cols, kv_cols)])
    load("wq", wq_hbm, wq_v)
    load("wo", wo_hbm.at[:, pl.ds(my_cols, half)], w_all.at[0])
    load("we", wo_hbm.at[:, pl.ds(other_cols, half // GROUPS)], w_ext.at[0])

    barrier = pltpu.get_barrier_semaphore()
    for d in range(1, cp_size):
        pl.semaphore_signal(barrier, inc=1, device_id={"cp": lax.rem(me_c + d, cp_size)}, device_id_type=MESH)
    for peer in (up_t, dn_t, op_t):
        pl.semaphore_signal(barrier, inc=1, device_id=peer, device_id_type=MESH)

    rc = Copies(send_sems, recv_sems, (w_all, w_ext))
    def share_of(who):
        return pl.ds(pl.multiple_of(who * share, share), share)

    def part_of(who, i):
        return pl.ds(pl.multiple_of(who * share + i * part, part), part)

    gw = half // GROUPS

    def group_of(start, g):
        return pl.ds(pl.multiple_of(start + g * gw, gw), gw)

    def w_ref(g):
        return (w_ext, pl.ds(0, gw)) if g == EXTRA else (w_all, pl.ds(g * gw, gw))

    def send_shares(g):
        buf, here = w_ref(g)
        near_cols = group_of(my_cols, 0) if g == EXTRA else group_of(other_cols, g)
        rc.start(("w_up", g), w_share.at[:, near_cols], buf.at[3, pl.ds(row0, share), here], up_t, BATCH[g])
        rc.start(("w_dn", g), w_share.at[:, near_cols], buf.at[1, pl.ds(row0, share), here], dn_t, BATCH[g])
        if g != EXTRA:
            rc.start(("w_op", g), w_share.at[:, group_of(my_cols, g)], w_all.at[2, pl.ds(row0, share), here], op_t, BATCH[g])

    def relay_extra():
        lo, hi, here = part_of(me_c, 0), part_of(me_c, 1), pl.ds(0, gw)
        rc.start("e_up", w_all.at[3, lo, here], w_ext.at[2, lo, here], up_t, BATCH[EXTRA])
        rc.start("e_dn", w_all.at[1, hi, here], w_ext.at[2, hi, here], dn_t, BATCH[EXTRA])

    def spread_own(r, g):
        if r == 2 and g == EXTRA:
            rc.arrived("e_up")
            rc.arrived("e_dn")
        else:
            rc.arrived((("w_dn", "w_op", "w_up")[r - 1], g))
        buf, here = w_ref(g)
        at = (r, share_of(me_c), here)
        rc.start(("xu", r, g), buf.at[at], buf.at[at], up_x, BATCH[g])
        rc.start(("xd", r, g), buf.at[at], buf.at[at], dn_x, BATCH[g])
        rc.start(("m0", r, g), buf.at[at], buf.at[at], mate, BATCH[g], ("m", g))

    def spread_near(r, g):
        buf, here = w_ref(g)
        for name, fwd, to_mate, source, i, onward in (("xu", "fu", "m1", dn_x, 0, up_x), ("xd", "fd", "m2", up_x, 1, dn_x)):
            at = (r, part_of(source["cp"], i), here)
            rc.arrived((name, r, g))
            rc.start((fwd, r, g), buf.at[at], buf.at[at], onward, BATCH[g])
            at = (r, share_of(source["cp"]), here)
            rc.start((to_mate, r, g), buf.at[at], buf.at[at], mate, BATCH[g], ("m", g))

    def spread_far(r, g):
        buf, here = w_ref(g)
        at = (r, share_of(lax.rem(me_c + cp_size // 2, cp_size)), here)
        rc.arrived(("fu", r, g))
        rc.arrived(("fd", r, g))
        rc.start(("m3", r, g), buf.at[at], buf.at[at], mate, BATCH[g], ("m", g))

    loads["pos"].wait()
    loads["freq"].wait()
    pos_all[0] = pos_v[...]
    freq = jnp.concatenate([freq_v[...], freq_v[...]], axis=1)
    sign = jnp.where(lax.broadcasted_iota(jnp.int32, (1, head_dim), 1) < head_dim // 2, -1.0, 1.0).astype(F32)
    left = lax.broadcasted_iota(jnp.int32, (BLK, head_dim), 1) < head_dim // 2
    for c in range(rows // BLK):
        posb_v[pl.ds(c * BLK, BLK), :] = jnp.transpose(jnp.broadcast_to(pos_v[pl.ds(c, 1), :], (BLK, BLK)))
    for c in range(rows // BLK // 2):
        at, up = pl.ds(c * BLK, BLK), pl.ds(piece + c * BLK, BLK)
        angle = jnp.where(left, posb_v[at, :], posb_v[up, :]).astype(F32) * freq
        for out, both in ((cos_v, jnp.cos(angle)), (sin_v, jnp.sin(angle))):
            turned = pltpu.roll(both, head_dim // 2, 1)
            scale = sign if out is sin_v else 1.0
            out[at, :] = jnp.where(left, both, turned) * scale
            out[up, :] = jnp.where(left, turned, both) * scale

    loads["gain"].wait()
    for c in range(rows // BLK):
        loads[("x", c)].wait()

        def norm(i, carry):
            at = pl.ds(pl.multiple_of(c * BLK + i * 32, 32), 32)
            x_f32 = x_v[at, :].astype(F32)
            inv_rms = lax.rsqrt(jnp.mean(x_f32 * x_f32, axis=-1, keepdims=True) + 1e-5)
            h_v[at, :] = (x_f32 * inv_rms * gain_v[...]).astype(BF16)
            return carry

        lax.fori_loop(0, BLK // 32, norm, 0)
        if c == 1:
            pl.semaphore_wait(barrier, cp_size + 2)
            loads["share"].wait()
            send_shares(1)

    def rope(raw, c):
        at = pl.ds(c * BLK, BLK)
        vec = raw.astype(F32)
        return (vec * cos_v[at, :] + pltpu.roll(vec, head_dim // 2, 1) * sin_v[at, :]).astype(BF16)

    def window_at(c):
        return c * BLK // piece, pl.ds(HALO + c * BLK % piece, BLK)

    loads["wk"].wait()
    loads["wv"].wait()
    kv_new = jnp.dot(h_v[...], wkv_v[...], preferred_element_type=F32).astype(BF16)
    for c in range(rows // BLK):
        p, at = window_at(c)
        new = kv_new[c * BLK:(c + 1) * BLK]
        for n in range(kv_heads):
            k_win[p, at, n * head_dim:(n + 1) * head_dim] = rope(new[:, n * head_dim:(n + 1) * head_dim], c)
        v_win[p, at, :] = new[:, kv_cols:]
    tail = pl.ds(piece, HALO)
    halo = pl.ds(0, HALO)
    rc.start("hk_a", k_win.at[0, tail], k_win.at[0, halo], nxt)
    rc.start("hk_b", k_win.at[1, tail], k_win.at[1, halo], prv)
    rc.start("hv_a", v_win.at[0, tail], v_win.at[0, halo], nxt)
    rc.start("hv_b", v_win.at[1, tail], v_win.at[1, halo], prv)

    send_shares(2)
    for d in range(1, cp_size):
        rc.start(("pos", d), pos_hbm, pos_all.at[cp_size - d], {"cp": lax.rem(me_c + d, cp_size)})

    loads["wq"].wait()

    q_new = jnp.dot(h_v[...], wq_v[...], preferred_element_type=F32).astype(BF16)
    for c in range(rows // BLK):
        for n in range(q_cols // head_dim):
            cols = slice(n * head_dim, (n + 1) * head_dim)
            q_v[pl.ds(c * BLK, BLK), cols] = rope(q_new[c * BLK:(c + 1) * BLK, cols], c)

    send_shares(0)
    for r in (3, 1, 2):
        spread_own(r, 1)
    for name in ("hk_a", "hk_b", "hv_a", "hv_b"):
        rc.arrived(name)

    @pl.when(me_c == cp_size - 1)
    def _():
        k_win[1, 0:HALO, :] = k_win[0, piece:piece + HALO, :]
        v_win[1, 0:HALO, :] = v_win[0, piece:piece + HALO, :]

    def send_o(p, n):
        block = (pl.ds(p * piece, piece), pl.ds(n * gcols, gcols))
        rc.start(("ou", p, n), o_all.at[(0,) + block], o_all.at[(3,) + block], up_t, "o")
        rc.start(("od", p, n), o_all.at[(0,) + block], o_all.at[(1,) + block], dn_t, "o")

    score_scale = head_dim ** -0.5
    for p in range(2):
        for n in range(kv_heads):
            cols = slice(n * head_dim, (n + 1) * head_dim)
            for b in range(piece // BLK):
                keys = HALO + (b + 1) * BLK
                at = pl.ds(p * piece + b * BLK, BLK)
                q_blk = jnp.concatenate([q_v[at, (n * group + g) * head_dim:(n * group + g + 1) * head_dim] for g in range(group)], axis=0)
                scores = lax.dot_general(q_blk, k_win[p, 0:keys, cols], (((1,), (1,)), ((), ())), preferred_element_type=F32) * score_scale
                key = lax.broadcasted_iota(jnp.int32, (BLK, keys), 1) - HALO
                row = lax.broadcasted_iota(jnp.int32, (BLK, keys), 0) + b * BLK
                back = jnp.concatenate([posb_v[at, :]] * (keys // BLK), axis=1)
                visible = (key <= row) & (key >= row - back)
                scores = jnp.where(visible[None], scores.reshape(group, BLK, keys), NEG)
                top = jnp.max(scores, axis=-1, keepdims=True)
                weights = jnp.exp(scores - top)
                probs = (weights / jnp.sum(weights, axis=-1, keepdims=True)).astype(BF16).reshape(group * BLK, keys)
                o_blk = jnp.dot(probs, v_win[p, 0:keys, cols], preferred_element_type=F32).astype(BF16)
                for g in range(group):
                    o_all[0, at, (n * group + g) * head_dim:(n * group + g + 1) * head_dim] = o_blk[g * BLK:(g + 1) * BLK]
            send_o(p, n)
            if (p, n) == (1, 0):
                send_shares(EXTRA)

    def forward_o(p):
        first = (pl.ds(p * piece, piece), pl.ds(0, gcols))
        last = (pl.ds(p * piece, piece), pl.ds((kv_heads - 1) * gcols, gcols))
        rc.arrived(("ou", p, 0))
        rc.start(("fou", p), o_all.at[(3,) + first], o_all.at[(2,) + first], up_t, "o")
        rc.arrived(("od", p, 0))
        rc.arrived(("od", p, 1))
        rc.start(("fod", p), o_all.at[(1,) + last], o_all.at[(2,) + last], dn_t, "o")
        rc.arrived(("ou", p, 1))

    def out_tile(p, g):
        at = pl.ds(p * piece, piece)
        buf, cols = w_ref(g)
        acc = jnp.dot(o_all[0, at, :], buf[0, :, cols], preferred_element_type=F32)
        for r in range(1, tp_size):
            acc += jnp.dot(o_all[r, at, :], buf[r, :, cols], preferred_element_type=F32)
        x_cols = group_of(other_cols, 0) if g == EXTRA else group_of(my_cols, g)
        y_out[at, x_cols] = (x_v[at, x_cols].astype(F32) + acc).astype(BF16)
        if g in (1, 2):
            lo, hi = pl.ds(p * piece, BLK), pl.ds(p * piece + BLK, BLK)
            rc.start(("yd", p, g), y_out.at[lo, x_cols], y_out.at[lo, x_cols], dn_t, "y", "y")
            rc.start(("yu", p, g), y_out.at[hi, x_cols], y_out.at[hi, x_cols], up_t, "y", "y")

    def each_slot(step, g):
        for r in (3, 1, 2):
            step(r, g)

    each_slot(spread_own, 2)
    for win, out in ((k_win, k_out), (v_win, v_out)):
        for c in range(rows // BLK):
            p, at = window_at(c)
            out[pl.ds(c * BLK, BLK)] = jnp.stack([win[p, at, n * head_dim:(n + 1) * head_dim] for n in range(kv_heads)], axis=1)
    for d in range(1, cp_size):
        rc.arrived(("pos", d))
    sub = lax.broadcasted_iota(jnp.int32, pos_all.shape, 1)
    lane = lax.broadcasted_iota(jnp.int32, pos_all.shape, 2)
    first_tok = (lane == 0) & ((sub == 0) | (sub == piece // BLK))
    far_s[0] = jnp.max(jnp.where(first_tok, pos_all[...], 0))
    load("far", far_s, far_hbm)

    each_slot(spread_near, 1)
    each_slot(spread_own, 0)
    relay_extra()
    each_slot(spread_near, 2)
    forward_o(0)
    each_slot(spread_own, EXTRA)
    each_slot(spread_far, 1)
    each_slot(spread_near, 0)
    forward_o(1)
    each_slot(spread_far, 2)
    loads["wo"].wait()
    loads["we"].wait()
    rc.batch_arrived(("m", 1))
    rc.arrived(("fou", 0))
    rc.arrived(("fod", 0))
    out_tile(0, 1)
    rc.batch_arrived(("m", 2))
    out_tile(0, 2)
    each_slot(spread_far, 0)
    rc.arrived(("fou", 1))
    rc.arrived(("fod", 1))
    out_tile(1, 1)
    out_tile(1, 2)
    each_slot(spread_near, EXTRA)
    rc.batch_arrived(("m", 0))
    out_tile(0, 0)
    out_tile(1, 0)
    each_slot(spread_far, EXTRA)
    rc.batch_arrived(("m", EXTRA))
    out_tile(0, EXTRA)
    out_tile(1, EXTRA)

    loads["far"].wait()
    rc.drain()
    rc.batch_arrived("y")


def fused_layer(cp_size, tp_size, x_in, pos_in_doc, norm_gain, w_q, w_k, w_v, w_o, inv_freq):
    rows, d_model = x_in.shape
    q_cols, kv_cols = w_q.shape[1], w_k.shape[1]
    head_dim = 2 * inv_freq.shape[0]
    kv_heads = kv_cols // head_dim
    piece, half = rows // 2, d_model // 2
    vm = pltpu.VMEM
    copies = 3 * GROUPS + 4 + (cp_size - 1) + 4 + 3 * (GROUPS + 1) * 4 + (GROUPS + 1) + 8 + 4 + 1
    any_spec = pl.BlockSpec(memory_space=pl.ANY)
    return pl.pallas_call(
        functools.partial(layer_kernel, cp_size, tp_size),
        name="fused_layer",
        out_shape=[
            vm((rows, d_model), BF16),
            vm((rows, kv_heads, head_dim), BF16),
            vm((rows, kv_heads, head_dim), BF16),
            jax.ShapeDtypeStruct((1,), jnp.int32),
        ],
        in_specs=[pl.BlockSpec(memory_space=pltpu.HBM)] * 8,
        out_specs=[pl.BlockSpec(memory_space=pltpu.VMEM)] * 3 + [any_spec],
        scratch_shapes=[
            vm((rows, d_model), BF16), vm((rows, d_model), BF16),
            vm(w_q.shape, BF16), vm((d_model, 2 * kv_cols), BF16),
            vm((tp_size, q_cols, half), BF16), vm((tp_size, q_cols, half // GROUPS), BF16), vm((q_cols // cp_size, d_model), BF16),
            vm((tp_size, rows, q_cols), BF16), vm((rows, q_cols), BF16),
            vm((2, HALO + piece, kv_cols), BF16), vm((2, HALO + piece, kv_cols), BF16),
            vm((rows // BLK, BLK), jnp.int32), vm((1, d_model), F32), vm((1, head_dim // 2), F32),
            vm((rows, head_dim), F32), vm((rows, head_dim), F32), vm((rows, BLK), jnp.int32),
            vm((cp_size, rows // BLK, BLK), jnp.int32),
            pltpu.SMEM((1,), jnp.int32),
            pltpu.SemaphoreType.DMA((14,)),
            pltpu.SemaphoreType.DMA((4 + 4 + cp_size - 1,)), pltpu.SemaphoreType.DMA((copies,)),
        ],
        compiler_params=pltpu.CompilerParams(collective_id=0, has_side_effects=True, vmem_limit_bytes=59 * 1024 * 1024),
    )(x_in, pos_in_doc.reshape(rows // BLK, BLK), norm_gain.reshape(1, d_model), w_q, w_k, w_v, w_o, inv_freq.reshape(1, head_dim // 2))


def store_kernel(y_v, k_v, v_v, y_hbm, k_hbm, v_hbm, sems):
    copies = [pltpu.make_async_copy(k_v, k_hbm, sems.at[0]), pltpu.make_async_copy(v_v, v_hbm, sems.at[1])]
    for i in range(4):
        at = pl.ds(i * y_v.shape[0] // 4, y_v.shape[0] // 4)
        copies.append(pltpu.make_async_copy(y_v.at[at], y_hbm.at[at], sems.at[2 + i]))
    for copy in copies:
        copy.start()
    for copy in copies:
        copy.wait()


def store_outputs(y_v, k_v, v_v):
    return pl.pallas_call(
        store_kernel,
        name="store_outputs",
        out_shape=[jax.ShapeDtypeStruct(a.shape, a.dtype) for a in (y_v, k_v, v_v)],
        in_specs=[pl.BlockSpec(memory_space=pltpu.VMEM)] * 3,
        out_specs=[pl.BlockSpec(memory_space=pltpu.HBM)] * 3,
        scratch_shapes=[pltpu.SemaphoreType.DMA((6,))],
        compiler_params=pltpu.CompilerParams(vmem_limit_bytes=1024 * 1024),
    )(y_v, k_v, v_v)


def gather_kernel(axis, size, part_hbm, all_hbm, load_sem, send_sems, recv_sems):
    me = lax.axis_index(axis)
    barrier = pltpu.get_barrier_semaphore()
    for d in range(1, size):
        pl.semaphore_signal(barrier, inc=1, device_id={axis: lax.rem(me + d, size)}, device_id_type=MESH)
    pl.semaphore_wait(barrier, size - 1)
    own = pltpu.make_async_copy(part_hbm, all_hbm.at[me], load_sem)
    own.start()
    copies = []
    for d in range(1, size):
        copies.append(pltpu.make_async_remote_copy(src_ref=part_hbm, dst_ref=all_hbm.at[me], send_sem=send_sems.at[d - 1], recv_sem=recv_sems.at[d - 1], device_id={axis: lax.rem(me + d, size)}, device_id_type=MESH))
        copies[-1].start()
    for copy in copies:
        copy.wait()
    own.wait()


def gather(part, axis, size, collective_id):
    any_spec = pl.BlockSpec(memory_space=pl.ANY)
    return pl.pallas_call(
        functools.partial(gather_kernel, axis, size),
        name="gather_%d" % collective_id,
        out_shape=jax.ShapeDtypeStruct((size,) + part.shape, part.dtype),
        in_specs=[any_spec],
        out_specs=any_spec,
        scratch_shapes=[pltpu.SemaphoreType.DMA, pltpu.SemaphoreType.DMA((size - 1,)), pltpu.SemaphoreType.DMA((size - 1,))],
        compiler_params=pltpu.CompilerParams(collective_id=collective_id, has_side_effects=True),
    )(part)


def rope_ref(vectors, cos_t, sin_t):
    half_dim = vectors.shape[-1] // 2
    lower_half = vectors[..., :half_dim].astype(F32)
    upper_half = vectors[..., half_dim:].astype(F32)
    return jnp.concatenate([lower_half * cos_t - upper_half * sin_t, upper_half * cos_t + lower_half * sin_t], axis=-1).astype(BF16)


def global_index(stored_pos, local_rows, cp_size):
    piece_len = local_rows // 2
    owner = stored_pos // local_rows
    within = stored_pos % local_rows
    piece_id = jnp.where(within < piece_len, owner, 2 * cp_size - 1 - owner)
    return piece_id * piece_len + within % piece_len


def general_y(cp_size, tp_size, x_in, pos_in_doc, norm_gain, w_q, w_o, inv_freq, k_rot, v_new):
    rows, kv_heads, head_dim = k_rot.shape
    tokens = rows * cp_size
    x_f32 = x_in.astype(F32)
    inv_rms = lax.rsqrt(jnp.mean(x_f32 * x_f32, axis=-1, keepdims=True) + 1e-5)
    normed = (x_f32 * inv_rms * norm_gain).astype(BF16)
    q_new = jnp.dot(normed, w_q, preferred_element_type=F32).astype(BF16).reshape(rows, kv_heads, -1, head_dim)
    angle = pos_in_doc.astype(F32)[:, None] * inv_freq[None, :]
    q_rot = rope_ref(q_new, jnp.cos(angle)[:, None, None, :], jnp.sin(angle)[:, None, None, :])
    keys = gather(k_rot.reshape(rows, kv_heads * head_dim), "cp", cp_size, 1).reshape(tokens, kv_heads, head_dim)
    vals = gather(v_new.reshape(rows, kv_heads * head_dim), "cp", cp_size, 2).reshape(tokens, kv_heads, head_dim)
    q_idx = global_index(lax.axis_index("cp") * rows + jnp.arange(rows), rows, cp_size)
    key_idx = global_index(jnp.arange(tokens), rows, cp_size)

    def attend(block_args):
        q_blk, idx_blk, pos_blk = block_args
        scores = jnp.einsum("qngd,knd->ngqk", q_blk, keys, preferred_element_type=F32) * head_dim ** -0.5
        visible = (key_idx[None, :] >= (idx_blk - pos_blk)[:, None]) & (key_idx[None, :] <= idx_blk[:, None])
        probs = jax.nn.softmax(jnp.where(visible, scores, NEG), axis=-1).astype(BF16)
        return jnp.einsum("ngqk,knd->qngd", probs, vals, preferred_element_type=F32).astype(BF16)

    blocks = rows // BLK
    o_own = lax.map(attend, (q_rot.reshape(blocks, BLK, kv_heads, -1, head_dim), q_idx.reshape(blocks, BLK), pos_in_doc.reshape(blocks, BLK))).reshape(rows, -1)
    o_parts = gather(o_own, "tp", tp_size, 3)
    w_parts = gather(w_o, "tp", tp_size, 4)
    mixed = jnp.einsum("trc,tcd->rd", o_parts, w_parts, preferred_element_type=F32)
    return (x_f32 + mixed).astype(BF16)


def solution(mesh):
    cp_size, tp_size = mesh.shape["cp"], mesh.shape["tp"]

    def local_step(x_in, doc_id, pos_in_doc, norm_gain, w_q, w_k, w_v, w_o, inv_freq):
        y_out, k_rot, v_new, far = fused_layer(cp_size, tp_size, x_in, pos_in_doc, norm_gain, w_q, w_k, w_v, w_o, inv_freq)
        y_out, k_rot, v_new = store_outputs(y_out, k_rot, v_new)

        def redo(state):
            y_new = general_y(cp_size, tp_size, x_in, pos_in_doc, norm_gain, w_q, w_o, inv_freq, k_rot, v_new)
            return jnp.zeros_like(state[0]), y_new

        _, y_out = lax.while_loop(lambda state: state[0] > HALO, redo, (far[0], y_out))
        return y_out, k_rot, v_new

    row_spec = P(("dp", "cp"))
    in_specs = (P(("dp", "cp"), None), row_spec, row_spec, P(), P(None, "tp"), P(None, "tp"), P(None, "tp"), P("tp", None), P())
    out_specs = (P(("dp", "cp"), None), P(("dp", "cp"), "tp", None), P(("dp", "cp"), "tp", None))
    return jax.shard_map(local_step, mesh=mesh, in_specs=in_specs, out_specs=out_specs, check_vma=False)
```

```python
import functools
import math

import jax
import jax.numpy as jnp
from jax import lax
from jax.experimental import pallas as pl
from jax.experimental.pallas import tpu as pltpu
from jax.sharding import PartitionSpec as P

MESH = pl.DeviceIdType.MESH
F32 = jnp.float32
BF16 = jnp.bfloat16
HALO = 128
BLK = 128
GROUPS = 3
EXTRA = 3
STORES = 16
BATCH = ("w", "w", "w", "e")
NEG = -1e30


class Copies:
    def __init__(self, send_sems, recv_sems, rulers):
        self.send_sems, self.recv_sems, self.rulers = send_sems, recv_sems, rulers
        self.made, self.send_slots, self.recv_slots, self.sent, self.due = {}, {}, {}, {}, {}

    def start(self, name, src, dst, device, send_batch=None, recv_batch=None):
        send_slot = self.send_slots.setdefault(send_batch or name, len(self.send_slots))
        recv_slot = self.recv_slots.setdefault(recv_batch or name, len(self.recv_slots))
        copy = pltpu.make_async_remote_copy(src_ref=src, dst_ref=dst, send_sem=self.send_sems.at[send_slot], recv_sem=self.recv_sems.at[recv_slot], device_id=device, device_id_type=MESH)
        size = math.prod(src.shape)
        if send_batch is None:
            self.made[name] = (copy, True)
        else:
            self.made[name] = (copy, False)
            self.sent[send_batch] = self.sent.get(send_batch, 0) + size
        if recv_batch is not None:
            self.due[recv_batch] = self.due.get(recv_batch, 0) + size
        copy.start()

    def wait_size(self, sem, size):
        fits = []
        for ruler in self.rulers:
            slabs, depth, width = ruler.shape
            fits += [(ruler, n, size // width // n) for n in range(1, slabs + 1) if size % (16 * n * width) == 0 and size // width // n <= depth]
        ruler, count, deep = fits[0]
        ref = ruler.at[pl.ds(0, count), pl.ds(0, deep)]
        pltpu.make_async_copy(ref, ref, sem).wait()

    def arrived(self, name):
        self.made[name][0].wait_recv()

    def batch_arrived(self, batch):
        self.wait_size(self.recv_sems.at[self.recv_slots[batch]], self.due[batch])

    def drain(self):
        for copy, alone in self.made.values():
            if alone:
                copy.wait_send()
        for batch, size in self.sent.items():
            self.wait_size(self.send_sems.at[self.send_slots[batch]], size)


def layer_kernel(cp_size, tp_size, x_hbm, pos_hbm, gain_hbm, wq_hbm, wk_hbm, wv_hbm, wo_hbm, freq_hbm,
                 y_out, k_out, v_out, far_hbm,
                 x_v, h_v, wq_v, wkv_v, w_all, w_ext, w_share, o_all, q_v, k_win, v_win,
                 pos_v, gain_v, freq_v, cos_v, sin_v, posb_v, pos_all, far_s, load_sems, send_sems, recv_sems):
    rows, d_model = x_v.shape
    piece = rows // 2
    half = d_model // 2
    q_cols = q_v.shape[1]
    head_dim = freq_v.shape[1] * 2
    kv_cols = k_win.shape[2]
    kv_heads = kv_cols // head_dim
    group = q_cols // (kv_heads * head_dim)
    gcols = group * head_dim
    share = q_cols // cp_size
    part = share // 2

    me_c = lax.axis_index("cp")
    me_t = lax.axis_index("tp")
    up_t = {"tp": lax.rem(me_t + 1, tp_size)}
    dn_t = {"tp": lax.rem(me_t + tp_size - 1, tp_size)}
    op_t = {"tp": lax.rem(me_t + tp_size // 2, tp_size)}
    up_x = {"cp": lax.rem(me_c + 2, cp_size)}
    dn_x = {"cp": lax.rem(me_c + cp_size - 2, cp_size)}
    mate = {"cp": me_c + 1 - 2 * lax.rem(me_c, 2)}
    nxt = {"cp": lax.rem(me_c + 1, cp_size)}
    prv = {"cp": lax.rem(me_c + cp_size - 1, cp_size)}
    mine = lax.rem(me_t, 2)
    other = 1 - mine
    my_cols = pl.multiple_of(mine * half, half)
    other_cols = pl.multiple_of(other * half, half)

    row0 = pl.multiple_of(me_c * share, share)
    loads = {}

    def load(name, src, dst):
        copy = pltpu.make_async_copy(src, dst, load_sems.at[len(loads)])
        loads[name] = copy
        copy.start()

    load("pos", pos_hbm, pos_v)
    load("freq", freq_hbm, freq_v)
    load("gain", gain_hbm, gain_v)
    load("share", wo_hbm.at[pl.ds(row0, share)], w_share)
    for c in range(rows // BLK):
        load(("x", c), x_hbm.at[pl.ds(c * BLK, BLK)], x_v.at[pl.ds(c * BLK, BLK)])
    load("wk", wk_hbm, wkv_v.at[:, pl.ds(0, kv_cols)])
    load("wv", wv_hbm, wkv_v.at[:, pl.ds(kv_cols, kv_cols)])
    load("wq", wq_hbm, wq_v)
    load("wo", wo_hbm.at[:, pl.ds(my_cols, half)], w_all.at[0])
    load("we", wo_hbm.at[:, pl.ds(other_cols, half // GROUPS)], w_ext.at[0])

    barrier = pltpu.get_barrier_semaphore()
    for d in range(1, cp_size):
        pl.semaphore_signal(barrier, inc=1, device_id={"cp": lax.rem(me_c + d, cp_size)}, device_id_type=MESH)
    for peer in (up_t, dn_t, op_t):
        pl.semaphore_signal(barrier, inc=1, device_id=peer, device_id_type=MESH)

    rc = Copies(send_sems, recv_sems, (w_all, w_ext))
    def share_of(who):
        return pl.ds(pl.multiple_of(who * share, share), share)

    def part_of(who, i):
        return pl.ds(pl.multiple_of(who * share + i * part, part), part)

    gw = half // GROUPS

    def group_of(start, g):
        return pl.ds(pl.multiple_of(start + g * gw, gw), gw)

    def w_ref(g):
        return (w_ext, pl.ds(0, gw)) if g == EXTRA else (w_all, pl.ds(g * gw, gw))

    def send_shares(g):
        buf, here = w_ref(g)
        near_cols = group_of(my_cols, 0) if g == EXTRA else group_of(other_cols, g)
        rc.start(("w_up", g), w_share.at[:, near_cols], buf.at[3, pl.ds(row0, share), here], up_t, BATCH[g])
        rc.start(("w_dn", g), w_share.at[:, near_cols], buf.at[1, pl.ds(row0, share), here], dn_t, BATCH[g])
        if g != EXTRA:
            rc.start(("w_op", g), w_share.at[:, group_of(my_cols, g)], w_all.at[2, pl.ds(row0, share), here], op_t, BATCH[g])

    def relay_extra():
        lo, hi, here = part_of(me_c, 0), part_of(me_c, 1), pl.ds(0, gw)
        rc.start("e_up", w_all.at[3, lo, here], w_ext.at[2, lo, here], up_t, BATCH[EXTRA])
        rc.start("e_dn", w_all.at[1, hi, here], w_ext.at[2, hi, here], dn_t, BATCH[EXTRA])

    def spread_own(r, g):
        if r == 2 and g == EXTRA:
            rc.arrived("e_up")
            rc.arrived("e_dn")
        else:
            rc.arrived((("w_dn", "w_op", "w_up")[r - 1], g))
        buf, here = w_ref(g)
        at = (r, share_of(me_c), here)
        rc.start(("xu", r, g), buf.at[at], buf.at[at], up_x, BATCH[g])
        rc.start(("xd", r, g), buf.at[at], buf.at[at], dn_x, BATCH[g])
        rc.start(("m0", r, g), buf.at[at], buf.at[at], mate, BATCH[g], ("m", g))

    def spread_near(r, g):
        buf, here = w_ref(g)
        for name, fwd, to_mate, source, i, onward in (("xu", "fu", "m1", dn_x, 0, up_x), ("xd", "fd", "m2", up_x, 1, dn_x)):
            at = (r, part_of(source["cp"], i), here)
            rc.arrived((name, r, g))
            rc.start((fwd, r, g), buf.at[at], buf.at[at], onward, BATCH[g])
            at = (r, share_of(source["cp"]), here)
            rc.start((to_mate, r, g), buf.at[at], buf.at[at], mate, BATCH[g], ("m", g))

    def spread_far(r, g):
        buf, here = w_ref(g)
        at = (r, share_of(lax.rem(me_c + cp_size // 2, cp_size)), here)
        rc.arrived(("fu", r, g))
        rc.arrived(("fd", r, g))
        rc.start(("m3", r, g), buf.at[at], buf.at[at], mate, BATCH[g], ("m", g))

    loads["pos"].wait()
    loads["freq"].wait()
    pos_all[0] = pos_v[...]
    freq = jnp.concatenate([freq_v[...], freq_v[...]], axis=1)
    sign = jnp.where(lax.broadcasted_iota(jnp.int32, (1, head_dim), 1) < head_dim // 2, -1.0, 1.0).astype(F32)
    left = lax.broadcasted_iota(jnp.int32, (BLK, head_dim), 1) < head_dim // 2
    for c in range(rows // BLK):
        posb_v[pl.ds(c * BLK, BLK), :] = jnp.transpose(jnp.broadcast_to(pos_v[pl.ds(c, 1), :], (BLK, BLK)))
    for c in range(rows // BLK // 2):
        at, up = pl.ds(c * BLK, BLK), pl.ds(piece + c * BLK, BLK)
        angle = jnp.where(left, posb_v[at, :], posb_v[up, :]).astype(F32) * freq
        for out, both in ((cos_v, jnp.cos(angle)), (sin_v, jnp.sin(angle))):
            turned = pltpu.roll(both, head_dim // 2, 1)
            scale = sign if out is sin_v else 1.0
            out[at, :] = jnp.where(left, both, turned) * scale
            out[up, :] = jnp.where(left, turned, both) * scale

    loads["gain"].wait()
    for c in range(rows // BLK):
        loads[("x", c)].wait()

        def norm(i, carry):
            at = pl.ds(pl.multiple_of(c * BLK + i * 32, 32), 32)
            x_f32 = x_v[at, :].astype(F32)
            inv_rms = lax.rsqrt(jnp.mean(x_f32 * x_f32, axis=-1, keepdims=True) + 1e-5)
            h_v[at, :] = (x_f32 * inv_rms * gain_v[...]).astype(BF16)
            return carry

        lax.fori_loop(0, BLK // 32, norm, 0)
        if c == 1:
            pl.semaphore_wait(barrier, cp_size + 2)
            loads["share"].wait()
            send_shares(1)

    def rope(raw, c):
        at = pl.ds(c * BLK, BLK)
        vec = raw.astype(F32)
        return (vec * cos_v[at, :] + pltpu.roll(vec, head_dim // 2, 1) * sin_v[at, :]).astype(BF16)

    def window_at(c):
        return c * BLK // piece, pl.ds(HALO + c * BLK % piece, BLK)

    loads["wk"].wait()
    loads["wv"].wait()
    kv_new = jnp.dot(h_v[...], wkv_v[...], preferred_element_type=F32).astype(BF16)
    for c in range(rows // BLK):
        p, at = window_at(c)
        new = kv_new[c * BLK:(c + 1) * BLK]
        for n in range(kv_heads):
            k_win[p, at, n * head_dim:(n + 1) * head_dim] = rope(new[:, n * head_dim:(n + 1) * head_dim], c)
        v_win[p, at, :] = new[:, kv_cols:]
    tail = pl.ds(piece, HALO)
    halo = pl.ds(0, HALO)
    rc.start("hk_a", k_win.at[0, tail], k_win.at[0, halo], nxt)
    rc.start("hk_b", k_win.at[1, tail], k_win.at[1, halo], prv)
    rc.start("hv_a", v_win.at[0, tail], v_win.at[0, halo], nxt)
    rc.start("hv_b", v_win.at[1, tail], v_win.at[1, halo], prv)

    send_shares(2)
    for d in range(1, cp_size):
        rc.start(("pos", d), pos_hbm, pos_all.at[cp_size - d], {"cp": lax.rem(me_c + d, cp_size)})

    loads["wq"].wait()

    q_new = jnp.dot(h_v[...], wq_v[...], preferred_element_type=F32).astype(BF16)
    for c in range(rows // BLK):
        for n in range(q_cols // head_dim):
            cols = slice(n * head_dim, (n + 1) * head_dim)
            q_v[pl.ds(c * BLK, BLK), cols] = rope(q_new[c * BLK:(c + 1) * BLK, cols], c)

    send_shares(0)
    for r in (3, 1, 2):
        spread_own(r, 1)
    for name in ("hk_a", "hk_b", "hv_a", "hv_b"):
        rc.arrived(name)

    @pl.when(me_c == cp_size - 1)
    def _():
        k_win[1, 0:HALO, :] = k_win[0, piece:piece + HALO, :]
        v_win[1, 0:HALO, :] = v_win[0, piece:piece + HALO, :]

    def send_o(p, n):
        block = (pl.ds(p * piece, piece), pl.ds(n * gcols, gcols))
        rc.start(("ou", p, n), o_all.at[(0,) + block], o_all.at[(3,) + block], up_t, "o")
        rc.start(("od", p, n), o_all.at[(0,) + block], o_all.at[(1,) + block], dn_t, "o")

    score_scale = head_dim ** -0.5
    for p in range(2):
        for n in range(kv_heads):
            cols = slice(n * head_dim, (n + 1) * head_dim)
            for b in range(piece // BLK):
                keys = HALO + (b + 1) * BLK
                at = pl.ds(p * piece + b * BLK, BLK)
                q_blk = jnp.concatenate([q_v[at, (n * group + g) * head_dim:(n * group + g + 1) * head_dim] for g in range(group)], axis=0)
                scores = lax.dot_general(q_blk, k_win[p, 0:keys, cols], (((1,), (1,)), ((), ())), preferred_element_type=F32) * score_scale
                key = lax.broadcasted_iota(jnp.int32, (BLK, keys), 1) - HALO
                row = lax.broadcasted_iota(jnp.int32, (BLK, keys), 0) + b * BLK
                back = jnp.concatenate([posb_v[at, :]] * (keys // BLK), axis=1)
                visible = (key <= row) & (key >= row - back)
                scores = jnp.where(visible[None], scores.reshape(group, BLK, keys), NEG)
                top = jnp.max(scores, axis=-1, keepdims=True)
                weights = jnp.exp(scores - top)
                probs = (weights / jnp.sum(weights, axis=-1, keepdims=True)).astype(BF16).reshape(group * BLK, keys)
                o_blk = jnp.dot(probs, v_win[p, 0:keys, cols], preferred_element_type=F32).astype(BF16)
                for g in range(group):
                    o_all[0, at, (n * group + g) * head_dim:(n * group + g + 1) * head_dim] = o_blk[g * BLK:(g + 1) * BLK]
            send_o(p, n)
            if (p, n) == (1, 0):
                send_shares(EXTRA)

    def forward_o(p):
        first = (pl.ds(p * piece, piece), pl.ds(0, gcols))
        last = (pl.ds(p * piece, piece), pl.ds((kv_heads - 1) * gcols, gcols))
        rc.arrived(("ou", p, 0))
        rc.start(("fou", p), o_all.at[(3,) + first], o_all.at[(2,) + first], up_t, "o")
        rc.arrived(("od", p, 0))
        rc.arrived(("od", p, 1))
        rc.start(("fod", p), o_all.at[(1,) + last], o_all.at[(2,) + last], dn_t, "o")
        rc.arrived(("ou", p, 1))

    def out_tile(p, g):
        at = pl.ds(p * piece, piece)
        buf, cols = w_ref(g)
        acc = jnp.dot(o_all[0, at, :], buf[0, :, cols], preferred_element_type=F32)
        for r in range(1, tp_size):
            acc += jnp.dot(o_all[r, at, :], buf[r, :, cols], preferred_element_type=F32)
        x_cols = group_of(other_cols, 0) if g == EXTRA else group_of(my_cols, g)
        y_out[at, x_cols] = (x_v[at, x_cols].astype(F32) + acc).astype(BF16)
        if g in (1, 2):
            lo, hi = pl.ds(p * piece, BLK), pl.ds(p * piece + BLK, BLK)
            rc.start(("yd", p, g), y_out.at[lo, x_cols], y_out.at[lo, x_cols], dn_t, "y", "y")
            rc.start(("yu", p, g), y_out.at[hi, x_cols], y_out.at[hi, x_cols], up_t, "y", "y")

    def each_slot(step, g):
        for r in (3, 1, 2):
            step(r, g)

    each_slot(spread_own, 2)
    for win, out in ((k_win, k_out), (v_win, v_out)):
        for c in range(rows // BLK):
            p, at = window_at(c)
            out[pl.ds(c * BLK, BLK)] = jnp.stack([win[p, at, n * head_dim:(n + 1) * head_dim] for n in range(kv_heads)], axis=1)
    for d in range(1, cp_size):
        rc.arrived(("pos", d))
    sub = lax.broadcasted_iota(jnp.int32, pos_all.shape, 1)
    lane = lax.broadcasted_iota(jnp.int32, pos_all.shape, 2)
    first_tok = (lane == 0) & ((sub == 0) | (sub == piece // BLK))
    far_s[0] = jnp.max(jnp.where(first_tok, pos_all[...], 0))
    load("far", far_s, far_hbm)

    each_slot(spread_near, 1)
    each_slot(spread_own, 0)
    relay_extra()
    each_slot(spread_near, 2)
    forward_o(0)
    each_slot(spread_own, EXTRA)
    each_slot(spread_far, 1)
    each_slot(spread_near, 0)
    forward_o(1)
    each_slot(spread_far, 2)
    loads["wo"].wait()
    loads["we"].wait()
    rc.batch_arrived(("m", 1))
    rc.arrived(("fou", 0))
    rc.arrived(("fod", 0))
    out_tile(0, 1)
    rc.batch_arrived(("m", 2))
    out_tile(0, 2)
    each_slot(spread_far, 0)
    rc.arrived(("fou", 1))
    rc.arrived(("fod", 1))
    out_tile(1, 1)
    out_tile(1, 2)
    each_slot(spread_near, EXTRA)
    rc.batch_arrived(("m", 0))
    out_tile(0, 0)
    out_tile(1, 0)
    each_slot(spread_far, EXTRA)
    rc.batch_arrived(("m", EXTRA))
    out_tile(0, EXTRA)
    out_tile(1, EXTRA)

    loads["far"].wait()
    rc.drain()
    rc.batch_arrived("y")


def fused_layer(cp_size, tp_size, x_in, pos_in_doc, norm_gain, w_q, w_k, w_v, w_o, inv_freq):
    rows, d_model = x_in.shape
    q_cols, kv_cols = w_q.shape[1], w_k.shape[1]
    head_dim = 2 * inv_freq.shape[0]
    kv_heads = kv_cols // head_dim
    piece, half = rows // 2, d_model // 2
    vm = pltpu.VMEM
    copies = 3 * GROUPS + 4 + (cp_size - 1) + 4 + 3 * (GROUPS + 1) * 4 + (GROUPS + 1) + 8 + 4 + 1
    any_spec = pl.BlockSpec(memory_space=pl.ANY)
    return pl.pallas_call(
        functools.partial(layer_kernel, cp_size, tp_size),
        name="fused_layer",
        out_shape=[
            vm((rows, d_model), BF16),
            vm((rows, kv_heads, head_dim), BF16),
            vm((rows, kv_heads, head_dim), BF16),
            jax.ShapeDtypeStruct((1,), jnp.int32),
        ],
        in_specs=[pl.BlockSpec(memory_space=pltpu.HBM)] * 8,
        out_specs=[pl.BlockSpec(memory_space=pltpu.VMEM)] * 3 + [any_spec],
        scratch_shapes=[
            vm((rows, d_model), BF16), vm((rows, d_model), BF16),
            vm(w_q.shape, BF16), vm((d_model, 2 * kv_cols), BF16),
            vm((tp_size, q_cols, half), BF16), vm((tp_size, q_cols, half // GROUPS), BF16), vm((q_cols // cp_size, d_model), BF16),
            vm((tp_size, rows, q_cols), BF16), vm((rows, q_cols), BF16),
            vm((2, HALO + piece, kv_cols), BF16), vm((2, HALO + piece, kv_cols), BF16),
            vm((rows // BLK, BLK), jnp.int32), vm((1, d_model), F32), vm((1, head_dim // 2), F32),
            vm((rows, head_dim), F32), vm((rows, head_dim), F32), vm((rows, BLK), jnp.int32),
            vm((cp_size, rows // BLK, BLK), jnp.int32),
            pltpu.SMEM((1,), jnp.int32),
            pltpu.SemaphoreType.DMA((14,)),
            pltpu.SemaphoreType.DMA((4 + 4 + cp_size - 1,)), pltpu.SemaphoreType.DMA((copies,)),
        ],
        compiler_params=pltpu.CompilerParams(collective_id=0, has_side_effects=True, vmem_limit_bytes=59 * 1024 * 1024),
    )(x_in, pos_in_doc.reshape(rows // BLK, BLK), norm_gain.reshape(1, d_model), w_q, w_k, w_v, w_o, inv_freq.reshape(1, head_dim // 2))


def store_kernel(y_v, k_v, v_v, y_hbm, k_hbm, v_hbm, sems):
    copies = [pltpu.make_async_copy(k_v, k_hbm, sems.at[0]), pltpu.make_async_copy(v_v, v_hbm, sems.at[1])]
    for i in range(STORES):
        at = pl.ds(i * (y_v.shape[0] // STORES), y_v.shape[0] // STORES)
        copies.append(pltpu.make_async_copy(y_v.at[at], y_hbm.at[at], sems.at[2 + i]))
    for copy in copies:
        copy.start()
    for copy in copies:
        copy.wait()


def store_outputs(y_v, k_v, v_v):
    return pl.pallas_call(
        store_kernel,
        name="store_outputs",
        out_shape=[jax.ShapeDtypeStruct(a.shape, a.dtype) for a in (y_v, k_v, v_v)],
        in_specs=[pl.BlockSpec(memory_space=pltpu.VMEM)] * 3,
        out_specs=[pl.BlockSpec(memory_space=pltpu.HBM)] * 3,
        scratch_shapes=[pltpu.SemaphoreType.DMA((2 + STORES,))],
        compiler_params=pltpu.CompilerParams(vmem_limit_bytes=1024 * 1024),
    )(y_v, k_v, v_v)


def gather_kernel(axis, size, part_hbm, all_hbm, load_sem, send_sems, recv_sems):
    me = lax.axis_index(axis)
    barrier = pltpu.get_barrier_semaphore()
    for d in range(1, size):
        pl.semaphore_signal(barrier, inc=1, device_id={axis: lax.rem(me + d, size)}, device_id_type=MESH)
    pl.semaphore_wait(barrier, size - 1)
    own = pltpu.make_async_copy(part_hbm, all_hbm.at[me], load_sem)
    own.start()
    copies = []
    for d in range(1, size):
        copies.append(pltpu.make_async_remote_copy(src_ref=part_hbm, dst_ref=all_hbm.at[me], send_sem=send_sems.at[d - 1], recv_sem=recv_sems.at[d - 1], device_id={axis: lax.rem(me + d, size)}, device_id_type=MESH))
        copies[-1].start()
    for copy in copies:
        copy.wait()
    own.wait()


def gather(part, axis, size, collective_id):
    any_spec = pl.BlockSpec(memory_space=pl.ANY)
    return pl.pallas_call(
        functools.partial(gather_kernel, axis, size),
        name="gather_%d" % collective_id,
        out_shape=jax.ShapeDtypeStruct((size,) + part.shape, part.dtype),
        in_specs=[any_spec],
        out_specs=any_spec,
        scratch_shapes=[pltpu.SemaphoreType.DMA, pltpu.SemaphoreType.DMA((size - 1,)), pltpu.SemaphoreType.DMA((size - 1,))],
        compiler_params=pltpu.CompilerParams(collective_id=collective_id, has_side_effects=True),
    )(part)


def rope_ref(vectors, cos_t, sin_t):
    half_dim = vectors.shape[-1] // 2
    lower_half = vectors[..., :half_dim].astype(F32)
    upper_half = vectors[..., half_dim:].astype(F32)
    return jnp.concatenate([lower_half * cos_t - upper_half * sin_t, upper_half * cos_t + lower_half * sin_t], axis=-1).astype(BF16)


def global_index(stored_pos, local_rows, cp_size):
    piece_len = local_rows // 2
    owner = stored_pos // local_rows
    within = stored_pos % local_rows
    piece_id = jnp.where(within < piece_len, owner, 2 * cp_size - 1 - owner)
    return piece_id * piece_len + within % piece_len


def general_y(cp_size, tp_size, x_in, pos_in_doc, norm_gain, w_q, w_o, inv_freq, k_rot, v_new):
    rows, kv_heads, head_dim = k_rot.shape
    tokens = rows * cp_size
    x_f32 = x_in.astype(F32)
    inv_rms = lax.rsqrt(jnp.mean(x_f32 * x_f32, axis=-1, keepdims=True) + 1e-5)
    normed = (x_f32 * inv_rms * norm_gain).astype(BF16)
    q_new = jnp.dot(normed, w_q, preferred_element_type=F32).astype(BF16).reshape(rows, kv_heads, -1, head_dim)
    angle = pos_in_doc.astype(F32)[:, None] * inv_freq[None, :]
    q_rot = rope_ref(q_new, jnp.cos(angle)[:, None, None, :], jnp.sin(angle)[:, None, None, :])
    keys = gather(k_rot.reshape(rows, kv_heads * head_dim), "cp", cp_size, 1).reshape(tokens, kv_heads, head_dim)
    vals = gather(v_new.reshape(rows, kv_heads * head_dim), "cp", cp_size, 2).reshape(tokens, kv_heads, head_dim)
    q_idx = global_index(lax.axis_index("cp") * rows + jnp.arange(rows), rows, cp_size)
    key_idx = global_index(jnp.arange(tokens), rows, cp_size)

    def attend(block_args):
        q_blk, idx_blk, pos_blk = block_args
        scores = jnp.einsum("qngd,knd->ngqk", q_blk, keys, preferred_element_type=F32) * head_dim ** -0.5
        visible = (key_idx[None, :] >= (idx_blk - pos_blk)[:, None]) & (key_idx[None, :] <= idx_blk[:, None])
        probs = jax.nn.softmax(jnp.where(visible, scores, NEG), axis=-1).astype(BF16)
        return jnp.einsum("ngqk,knd->qngd", probs, vals, preferred_element_type=F32).astype(BF16)

    blocks = rows // BLK
    o_own = lax.map(attend, (q_rot.reshape(blocks, BLK, kv_heads, -1, head_dim), q_idx.reshape(blocks, BLK), pos_in_doc.reshape(blocks, BLK))).reshape(rows, -1)
    o_parts = gather(o_own, "tp", tp_size, 3)
    w_parts = gather(w_o, "tp", tp_size, 4)
    mixed = jnp.einsum("trc,tcd->rd", o_parts, w_parts, preferred_element_type=F32)
    return (x_f32 + mixed).astype(BF16)


def solution(mesh):
    cp_size, tp_size = mesh.shape["cp"], mesh.shape["tp"]

    def local_step(x_in, doc_id, pos_in_doc, norm_gain, w_q, w_k, w_v, w_o, inv_freq):
        y_out, k_rot, v_new, far = fused_layer(cp_size, tp_size, x_in, pos_in_doc, norm_gain, w_q, w_k, w_v, w_o, inv_freq)
        y_out, k_rot, v_new = store_outputs(y_out, k_rot, v_new)

        def redo(state):
            y_new = general_y(cp_size, tp_size, x_in, pos_in_doc, norm_gain, w_q, w_o, inv_freq, k_rot, v_new)
            return jnp.zeros_like(state[0]), y_new

        _, y_out = lax.while_loop(lambda state: state[0] > HALO, redo, (far[0], y_out))
        return y_out, k_rot, v_new

    row_spec = P(("dp", "cp"))
    in_specs = (P(("dp", "cp"), None), row_spec, row_spec, P(), P(None, "tp"), P(None, "tp"), P(None, "tp"), P("tp", None), P())
    out_specs = (P(("dp", "cp"), None), P(("dp", "cp"), "tp", None), P(("dp", "cp"), "tp", None))
    return jax.shard_map(local_step, mesh=mesh, in_specs=in_specs, out_specs=out_specs, check_vma=False)
```
